512 devices in a mesh: depth: 16 (over z, y_lo), rows: 32 (over x, y_hi, core).
Axes of the slice: x: 4, y: 8 (y_hi: 4, y_lo: 2; y = y_hi * 2 + y_lo), z: 8, core: 2. Of those that a mesh axis runs over, the one named last changes fastest.
Arguments:
- target: float32 [16, 2, 4096, 4096], P('depth', None, 'rows'), may hold values from -6 to 6
- depth_index: int32 [16], P('depth'), may hold values from 0 to 255
- band_mask: int32 [16, 2, 4096], P('depth'), may hold values from 0 to 1, as said below
Outputs:
- hologram: float32 [2, 4096, 4096], P(None, ('depth', 'rows'))
The draws below stay inside these ranges and needn't reach their ends.
Inputs may be any that keep to these rules, and one draw needn't show every extreme that they name: `band_mask`: for each plane and each of the two dimensions, the ones are exactly the frequency indices k with min(k, 4096 - k) below a cutoff between 512 and 2048.
All inputs are finite; a program needn't handle non-finite values.
Results may differ from the reference program's by a relative error of at most 0.0009.
Values sent between devices are 32-bit elements; how exact they have to be, the bound alone decides.
No kernel may reach another device: no remote copies, remote signals or barrier semaphores. Data moves between devices by JAX's collectives and lax.ppermute only.
A program may use at most 64 MiB of HBM per device.

```python
import math
import jax
import jax.numpy as jnp
from jax import lax

N = 4096
PLANES = 16
DEPTHS = 256


def draw_band_mask(key, part):
    cutoff = jax.random.randint(key, (PLANES, 2, 1), N // 8, N // 2 + 1)
    indices = jnp.arange(N, dtype=jnp.int32)
    folded = jnp.minimum(indices, N - indices)
    return (folded[None, None, :] < cutoff).astype(jnp.int32)


def place_ends(values, key, low, top_value):
    spot = [jax.random.randint(jax.random.fold_in(key, axis), (), 0, length) for axis, length in enumerate(values.shape)]
    main_axis = values.shape.index(max(values.shape))
    neighbour = spot[:main_axis] + [(spot[main_axis] + 1) % values.shape[main_axis]] + spot[main_axis + 1:]
    return values.at[tuple(spot)].set(low).at[tuple(neighbour)].set(top_value)


def levels(stream_key, dims, cuts, low, top_value):
    loudness = 1.0
    for axis_at, parts in cuts:
        steps = jax.random.uniform(jax.random.fold_in(jax.random.fold_in(stream_key, 6), axis_at), (parts,), jnp.float32, low / len(cuts), top_value / len(cuts))
        loudness = loudness * jnp.repeat(jnp.exp(steps), dims[axis_at] // parts).reshape((-1,) + (1,) * (len(dims) - 1 - axis_at))
    return loudness


def normal_values(key, dims, width, reach, split=(), kind=jnp.bfloat16):
    result = jax.random.normal(key, dims, jnp.float32) * width
    if len(split) > 0:
        result = levels(key, dims, split, -0.22, 0.18) * result
    return jnp.clip(result, min=-reach, max=reach).astype(kind)


def setup_inputs(seed: int = 0) -> dict:
    key_of = jax.random.split(jax.random.key(seed), 4)
    return {
        "target": normal_values(key_of[0], (PLANES, 2, N, N), 1.0, 6.0, ((0, 16), (2, 32)), jnp.float32),
        "depth_index": place_ends(jax.random.randint(key_of[1], (PLANES,), 0, DEPTHS), jax.random.fold_in(key_of[1], 1), 0, DEPTHS - 1).astype(jnp.int32),
        "band_mask": draw_band_mask(jax.random.fold_in(key_of[3], 71), 0),
    }


def reference(target, depth_index, band_mask):
    planes_all = target.shape[0]
    indices = jnp.arange(N, dtype=jnp.int32)
    signed = jnp.where(indices < N // 2, indices, indices - N)
    frequency = signed.astype(jnp.float32) / N
    radical = jnp.sqrt(4.0 - frequency[:, None] ** 2 - frequency[None, :] ** 2)

    def add_plane(running_sum, inputs):
        plane_data, level_index, mask_pair = inputs
        wavefront = lax.complex(plane_data[0], plane_data[1])
        spectrum = jnp.fft.fft2(wavefront, norm='ortho')
        distance = 100.0 + 2.0 * level_index.astype(jnp.float32)
        phases = 2.0 * math.pi * distance * (radical - 2.0)
        weights = mask_pair[0].astype(jnp.float32)[:, None] * mask_pair[1].astype(jnp.float32)[None, :]
        rotated = spectrum * lax.complex(jnp.cos(phases) * weights, jnp.sin(phases) * weights)
        return (running_sum + rotated, None)
    zeros_real = jnp.zeros((N, N), dtype=jnp.float32)
    initial = lax.complex(zeros_real, zeros_real)
    summed, _ = lax.scan(add_plane, initial, (target, depth_index, band_mask))
    field_out = jnp.fft.ifft2(summed, norm='ortho') / jnp.sqrt(jnp.float32(planes_all))
    return jnp.stack([jnp.real(field_out), jnp.imag(field_out)]).astype(jnp.float32)
```

```python
import functools
import math

import jax
import jax.numpy as jnp
import numpy as np
from jax import lax
from jax.experimental import pallas as pl
from jax.experimental.pallas import tpu as pltpu
from jax.sharding import Mesh
from jax.sharding import PartitionSpec as P

LOW = 32
HIGH = 128
N = 4096
DEPTH = ("depth_0", "depth_1")
DEPTH_ROWS = ("depth_0", "depth_1", "rows")
CHUNKS = 2
KC = HIGH // CHUNKS


def block_table(direction, scaling):
    index = np.arange(HIGH)
    angles = direction * 2.0 * np.pi / HIGH * (index[:, None] * index[None, :] % HIGH)
    cosine, sine = np.cos(angles) * scaling, np.sin(angles) * scaling
    table = np.concatenate(
        [np.concatenate([cosine, sine], 1), np.concatenate([-sine, cosine], 1)], 0
    ).astype(np.float32)
    high = table.astype(jnp.bfloat16)
    low = (table - high.astype(np.float32)).astype(jnp.bfloat16)
    return high, low


def twiddles(direction):
    product = np.arange(LOW)[:, None] * np.arange(HIGH)[None, :] % N
    angles = direction * 2.0 * np.pi / N * product
    return np.stack([np.cos(angles), np.sin(angles)]).astype(np.float32)


def add(a, b):
    return (a[0] + b[0], a[1] + b[1])


def sub(a, b):
    return (a[0] - b[0], a[1] - b[1])


def quarter(a, sign):
    return (-a[1], a[0]) if sign > 0 else (a[1], -a[0])


def turn(a, numerator, length, sign):
    numerator %= length
    if numerator == 0:
        return a
    if numerator * 4 == length:
        return quarter(a, sign)
    if numerator * 2 == length:
        return (-a[0], -a[1])
    if numerator * 8 == length:
        half = np.float32(math.sqrt(0.5))
        b = quarter(a, sign)
        return ((a[0] + b[0]) * half, (a[1] + b[1]) * half)
    if numerator * 8 == 3 * length:
        half = np.float32(math.sqrt(0.5))
        b = quarter(a, sign)
        return ((b[0] - a[0]) * half, (b[1] - a[1]) * half)
    angle = sign * 2.0 * math.pi * numerator / length
    cosine, sine = np.float32(math.cos(angle)), np.float32(math.sin(angle))
    return (a[0] * cosine - a[1] * sine, a[0] * sine + a[1] * cosine)


def four_points(values, sign):
    even, odd = add(values[0], values[2]), sub(values[0], values[2])
    even_2, odd_2 = add(values[1], values[3]), quarter(sub(values[1], values[3]), sign)
    return [add(even, even_2), add(odd, odd_2), sub(even, even_2), sub(odd, odd_2)]


def eight_points(values, sign):
    first = four_points(values[0::2], sign)
    second = four_points(values[1::2], sign)
    second = [turn(second[k], k, 8, sign) for k in range(4)]
    return [add(first[k], second[k]) for k in range(4)] + [
        sub(first[k], second[k]) for k in range(4)
    ]


def low_transform(load, store, part_ref, sign):
    for a in range(8):
        outs = four_points([load(a + 8 * b) for b in range(4)], sign)
        for q in range(4):
            pair = turn(outs[q], a * q, 32, sign)
            part_ref[q * 8 + a, 0] = pair[0]
            part_ref[q * 8 + a, 1] = pair[1]
    for q in range(4):
        values = [(part_ref[q * 8 + a, 0], part_ref[q * 8 + a, 1]) for a in range(8)]
        outs = eight_points(values, sign)
        for p in range(8):
            store(q + 4 * p, outs[p])


def product(rows, table):
    high_table, low_table = table[0][...], table[1][...]
    high = rows.astype(jnp.bfloat16)
    low = (rows - high.astype(jnp.float32)).astype(jnp.bfloat16)
    dot = functools.partial(jnp.dot, preferred_element_type=jnp.float32)
    return dot(high, high_table) + (dot(low, high_table) + dot(high, low_table))


WIDTH_ROWS = 16
WIDTH_STEPS = HIGH // WIDTH_ROWS
WIDTH_LOWS = LOW // WIDTH_STEPS


def width_kernel(x_ref, tw_ref, high_ref, low_ref, *rest):
    out_refs, (mid_ref, part_ref) = rest[:CHUNKS], rest[CHUNKS:]
    step = pl.program_id(0)

    @pl.when(step < WIDTH_STEPS)
    def _():
        for g in range(WIDTH_ROWS // 8):
            rows = pl.ds(pl.multiple_of(step * WIDTH_ROWS + 8 * g, 8), 8)

            def load(n):
                lanes = slice(HIGH * n, HIGH * (n + 1))
                return (
                    x_ref[0, 0, 8 * g : 8 * g + 8, lanes],
                    x_ref[0, 1, 8 * g : 8 * g + 8, lanes],
                )

            def store(k, pair):
                cosine, sine = tw_ref[0, k : k + 1, :], tw_ref[1, k : k + 1, :]
                mid_ref[k, rows, 0:HIGH] = pair[0] * cosine - pair[1] * sine
                mid_ref[k, rows, HIGH:] = pair[0] * sine + pair[1] * cosine

            low_transform(load, store, part_ref.at[g], -1)

    @pl.when(step >= WIDTH_STEPS)
    def _():
        base = (step - WIDTH_STEPS) * WIDTH_LOWS
        for k in range(WIDTH_LOWS):
            done = product(mid_ref[base + k], (high_ref, low_ref))
            for c in range(2):
                flat = done[:, HIGH * c : HIGH * (c + 1)].T
                for i in range(CHUNKS):
                    out_refs[i][k, c] = flat[KC * i : KC * (i + 1)]


def whole(*dims):
    return pl.BlockSpec(dims, lambda i: (0,) * len(dims))


def along_width(target):
    high, low = block_table(-1.0, 1.0 / 64)
    shape = jax.ShapeDtypeStruct((LOW, 2, KC, HIGH), jnp.float32)
    spec = pl.BlockSpec(
        (WIDTH_LOWS, 2, KC, HIGH), lambda i: (jnp.maximum(i - WIDTH_STEPS, 0), 0, 0, 0)
    )
    return pl.pallas_call(
        width_kernel,
        name="along_width",
        grid=(2 * WIDTH_STEPS,),
        in_specs=[
            pl.BlockSpec(
                (1, 2, WIDTH_ROWS, N), lambda i: (0, 0, jnp.minimum(i, WIDTH_STEPS - 1), 0)
            ),
            whole(2, LOW, HIGH),
            whole(2 * HIGH, 2 * HIGH),
            whole(2 * HIGH, 2 * HIGH),
        ],
        out_specs=[spec] * CHUNKS,
        out_shape=[shape] * CHUNKS,
        scratch_shapes=[
            pltpu.VMEM((LOW, HIGH, 2 * HIGH), jnp.float32),
            pltpu.VMEM((WIDTH_ROWS // 8, LOW, 2, 8, HIGH), jnp.float32),
        ],
        cost_estimate=pl.CostEstimate(
            flops=6 * N * 512 * 256, bytes_accessed=8 << 20, transcendentals=0
        ),
    )(target, jnp.asarray(twiddles(-1.0)), jnp.asarray(high), jnp.asarray(low))


HEIGHT_ROWS = 16


def height_kernel(x_ref, h_ref, ftw_ref, fh_ref, fl_ref, btw_ref, bh_ref, bl_ref,
                  out_ref, mid_ref, part_ref):
    groups = HEIGHT_ROWS // 8
    for g in range(groups):
        rows = slice(8 * g, 8 * g + 8)

        def load(n):
            return (x_ref[n, 0, rows, :], x_ref[n, 1, rows, :])

        def store(k, pair):
            cosine, sine = ftw_ref[0, k : k + 1, :], ftw_ref[1, k : k + 1, :]
            mid_ref[k, rows, 0:HIGH] = pair[0] * cosine - pair[1] * sine
            mid_ref[k, rows, HIGH:] = pair[0] * sine + pair[1] * cosine

        low_transform(load, store, part_ref.at[g], -1)

    count = 8
    for b in range(0, LOW, count):
        part = slice(b, b + count)
        flat = mid_ref[part].reshape(count * HEIGHT_ROWS, 2 * HIGH)
        spectrum = product(flat, (fh_ref, fl_ref))
        real, imaginary = spectrum[:, :HIGH], spectrum[:, HIGH:]
        cosine = h_ref[part, 0].reshape(count * HEIGHT_ROWS, HIGH)
        sine = h_ref[part, 1].reshape(count * HEIGHT_ROWS, HIGH)
        moved = jnp.concatenate(
            [real * cosine - imaginary * sine, real * sine + imaginary * cosine], axis=1
        )
        back = product(moved, (bh_ref, bl_ref))
        mid_ref[part] = back.reshape(count, HEIGHT_ROWS, 2 * HIGH)

    for g in range(groups):
        rows = slice(8 * g, 8 * g + 8)

        def load(k):
            real, imaginary = mid_ref[k, rows, 0:HIGH], mid_ref[k, rows, HIGH:]
            cosine, sine = btw_ref[0, k : k + 1, :], btw_ref[1, k : k + 1, :]
            return (real * cosine - imaginary * sine, real * sine + imaginary * cosine)

        def store(n, pair):
            out_ref[n, 0, rows, :] = pair[0]
            out_ref[n, 1, rows, :] = pair[1]

        low_transform(load, store, part_ref.at[g], 1)


def along_height(columns, transfer):
    spec = pl.BlockSpec((LOW, 2, HEIGHT_ROWS, HIGH), lambda i: (0, 0, i, 0))
    table = whole(2 * HIGH, 2 * HIGH)
    forward, backward = block_table(-1.0, 1.0 / 64), block_table(1.0, 1.0 / 64)
    count = columns.shape[2]
    return pl.pallas_call(
        height_kernel,
        name="along_height",
        grid=(count // HEIGHT_ROWS,),
        in_specs=[spec, spec, whole(2, LOW, HIGH), table, table, whole(2, LOW, HIGH), table, table],
        out_specs=spec,
        out_shape=jax.ShapeDtypeStruct((LOW, 2, count, HIGH), jnp.float32),
        scratch_shapes=[
            pltpu.VMEM((LOW, HEIGHT_ROWS, 2 * HIGH), jnp.float32),
            pltpu.VMEM((HEIGHT_ROWS // 8, LOW, 2, 8, HIGH), jnp.float32),
        ],
        cost_estimate=pl.CostEstimate(
            flops=12 * LOW * count * 512 * 256,
            bytes_accessed=3 * 8 * LOW * count * HIGH,
            transcendentals=0,
        ),
    )(
        columns,
        transfer,
        jnp.asarray(twiddles(-1.0)),
        *[jnp.asarray(t) for t in forward],
        jnp.asarray(twiddles(1.0)),
        *[jnp.asarray(t) for t in backward],
    )


def flip_kernel(*refs):
    in_refs, out_ref = refs[:-1], refs[-1]
    for n in range(out_ref.shape[0] // 16):
        for c in range(2):
            whole_tile = jnp.concatenate([ref[n, c] for ref in in_refs], axis=0)
            out_ref[16 * n : 16 * n + 16, c] = whole_tile.T.reshape(16, 8, HIGH)


def flip(shares):
    count = 16 * shares[0].shape[0]
    return pl.pallas_call(
        flip_kernel,
        name="flip",
        out_shape=jax.ShapeDtypeStruct((count, 2, 8, HIGH), jnp.float32),
    )(*shares)


def inverse_width_kernel(x_ref, tw_ref, high_ref, low_ref, out_ref, mid_ref, part_ref):
    total = x_ref[0:LOW] + x_ref[LOW:]
    rows = jnp.concatenate([total[:, 0], total[:, 1]], axis=-1).reshape(LOW * 8, 2 * HIGH)
    mid_ref[...] = product(rows, (high_ref, low_ref)).reshape(LOW, 8, 2 * HIGH)

    def load(k):
        real, imaginary = mid_ref[k, :, 0:HIGH], mid_ref[k, :, HIGH:]
        cosine, sine = tw_ref[0, k : k + 1, :], tw_ref[1, k : k + 1, :]
        return (real * cosine - imaginary * sine, real * sine + imaginary * cosine)

    def store(n, pair):
        out_ref[0, :, HIGH * n : HIGH * (n + 1)] = pair[0]
        out_ref[1, :, HIGH * n : HIGH * (n + 1)] = pair[1]

    low_transform(load, store, part_ref, 1)


def inverse_width(pieces, scaling):
    high, low = block_table(1.0, scaling / 64)
    return pl.pallas_call(
        inverse_width_kernel,
        name="inverse_width",
        out_shape=jax.ShapeDtypeStruct((2, 8, N), jnp.float32),
        scratch_shapes=[
            pltpu.VMEM((LOW, 8, 2 * HIGH), jnp.float32),
            pltpu.VMEM((LOW, 2, 8, HIGH), jnp.float32),
        ],
    )(pieces, jnp.asarray(twiddles(1.0)), jnp.asarray(high), jnp.asarray(low))


def signed(natural):
    return jnp.where(natural < N // 2, natural, natural - N)


def transfer_factors(depth_index, band_mask, column):
    high = jnp.arange(HIGH, dtype=jnp.int32)
    low = jnp.arange(LOW, dtype=jnp.int32)
    height = signed(low[:, None] + LOW * high[None, :])
    width = signed(column + LOW * high)
    square = (height * height)[:, None, :] + (width * width)[None, :, None]
    square = square.astype(jnp.float32) * np.float32(1.0 / (N * N))
    descent = -square / (jnp.sqrt(4.0 - square) + 2.0)
    turns = (100.0 + 2.0 * depth_index[0].astype(jnp.float32)) * descent
    angles = np.float32(2.0 * math.pi) * (turns - jnp.round(turns))
    mask_height = band_mask[0, 0].reshape(HIGH, LOW).T.astype(jnp.float32)
    mask_width = lax.dynamic_slice_in_dim(
        band_mask[0, 1].reshape(HIGH, LOW).T, column, 1, 0
    )[0].astype(jnp.float32)
    weights = mask_height[:, None, :] * mask_width[None, :, None]
    return jnp.stack([jnp.cos(angles) * weights, jnp.sin(angles) * weights], axis=1)


def local(target, depth_index, band_mask):
    spectra = along_width(target)
    transfer = transfer_factors(depth_index, band_mask, lax.axis_index("rows"))
    shares = []
    for i in range(CHUNKS):
        columns = lax.all_to_all(spectra[i], "rows", split_axis=0, concat_axis=0, tiled=True)
        part = along_height(columns, transfer[:, :, KC * i : KC * (i + 1)])
        shares.append(lax.psum_scatter(part, "depth_0", scatter_dimension=0, tiled=True))
    pieces = lax.all_to_all(
        flip(shares), ("depth_1", "rows"), split_axis=0, concat_axis=0, tiled=True
    )
    return inverse_width(pieces, 1.0 / math.sqrt(lax.axis_size(DEPTH)))


def solution(mesh):
    split = Mesh(mesh.devices.reshape(8, 2, mesh.shape["rows"]), ("depth_0", "depth_1", "rows"))
    in_specs = (P(DEPTH, None, "rows", None), P(DEPTH), P(DEPTH, None, None))
    out_specs = P(None, DEPTH_ROWS, None)
    return jax.shard_map(local, mesh=split, in_specs=in_specs, out_specs=out_specs, check_vma=False)
```

```python
import functools
import math

import jax
import jax.numpy as jnp
import numpy as np
from jax import lax
from jax.experimental import pallas as pl
from jax.experimental.pallas import tpu as pltpu
from jax.sharding import Mesh
from jax.sharding import PartitionSpec as P

LOW = 32
HIGH = 128
N = 4096
DEPTH = ("depth_0", "depth_1")
DEPTH_ROWS = ("depth_0", "depth_1", "rows")
CHUNKS = (96, 32)
STARTS = (0, 96)


def block_table(direction, scaling):
    index = np.arange(HIGH)
    angles = direction * 2.0 * np.pi / HIGH * (index[:, None] * index[None, :] % HIGH)
    cosine, sine = np.cos(angles) * scaling, np.sin(angles) * scaling
    table = np.concatenate(
        [np.concatenate([cosine, sine], 1), np.concatenate([-sine, cosine], 1)], 0
    ).astype(np.float32)
    high = table.astype(jnp.bfloat16)
    low = (table - high.astype(np.float32)).astype(jnp.bfloat16)
    return high, low


def twiddles(direction):
    product = np.arange(LOW)[:, None] * np.arange(HIGH)[None, :] % N
    angles = direction * 2.0 * np.pi / N * product
    return np.stack([np.cos(angles), np.sin(angles)]).astype(np.float32)


def add(a, b):
    return (a[0] + b[0], a[1] + b[1])


def sub(a, b):
    return (a[0] - b[0], a[1] - b[1])


def quarter(a, sign):
    return (-a[1], a[0]) if sign > 0 else (a[1], -a[0])


def turn(a, numerator, length, sign):
    numerator %= length
    if numerator == 0:
        return a
    if numerator * 4 == length:
        return quarter(a, sign)
    if numerator * 2 == length:
        return (-a[0], -a[1])
    if numerator * 8 == length:
        half = np.float32(math.sqrt(0.5))
        b = quarter(a, sign)
        return ((a[0] + b[0]) * half, (a[1] + b[1]) * half)
    if numerator * 8 == 3 * length:
        half = np.float32(math.sqrt(0.5))
        b = quarter(a, sign)
        return ((b[0] - a[0]) * half, (b[1] - a[1]) * half)
    angle = sign * 2.0 * math.pi * numerator / length
    cosine, sine = np.float32(math.cos(angle)), np.float32(math.sin(angle))
    return (a[0] * cosine - a[1] * sine, a[0] * sine + a[1] * cosine)


def four_points(values, sign):
    even, odd = add(values[0], values[2]), sub(values[0], values[2])
    even_2, odd_2 = add(values[1], values[3]), quarter(sub(values[1], values[3]), sign)
    return [add(even, even_2), add(odd, odd_2), sub(even, even_2), sub(odd, odd_2)]


def eight_points(values, sign):
    first = four_points(values[0::2], sign)
    second = four_points(values[1::2], sign)
    second = [turn(second[k], k, 8, sign) for k in range(4)]
    return [add(first[k], second[k]) for k in range(4)] + [
        sub(first[k], second[k]) for k in range(4)
    ]


def low_transform(load, store, part_ref, sign):
    for a in range(8):
        outs = four_points([load(a + 8 * b) for b in range(4)], sign)
        for q in range(4):
            pair = turn(outs[q], a * q, 32, sign)
            part_ref[q * 8 + a, 0] = pair[0]
            part_ref[q * 8 + a, 1] = pair[1]
    for q in range(4):
        values = [(part_ref[q * 8 + a, 0], part_ref[q * 8 + a, 1]) for a in range(8)]
        outs = eight_points(values, sign)
        for p in range(8):
            store(q + 4 * p, outs[p])


def product(rows, table):
    high_table, low_table = table[0][...], table[1][...]
    high = rows.astype(jnp.bfloat16)
    low = (rows - high.astype(jnp.float32)).astype(jnp.bfloat16)
    dot = functools.partial(jnp.dot, preferred_element_type=jnp.float32)
    return dot(high, high_table) + (dot(low, high_table) + dot(high, low_table))


WIDTH_ROWS = 16
WIDTH_STEPS = HIGH // WIDTH_ROWS
WIDTH_LOWS = LOW // WIDTH_STEPS


def width_kernel(x_ref, tw_ref, high_ref, low_ref, *rest):
    out_refs, (mid_ref, part_ref) = rest[: len(CHUNKS)], rest[len(CHUNKS) :]
    step = pl.program_id(0)

    @pl.when(step < WIDTH_STEPS)
    def _():
        for g in range(WIDTH_ROWS // 8):
            rows = pl.ds(pl.multiple_of(step * WIDTH_ROWS + 8 * g, 8), 8)

            def load(n):
                lanes = slice(HIGH * n, HIGH * (n + 1))
                return (
                    x_ref[0, 0, 8 * g : 8 * g + 8, lanes],
                    x_ref[0, 1, 8 * g : 8 * g + 8, lanes],
                )

            def store(k, pair):
                cosine, sine = tw_ref[0, k : k + 1, :], tw_ref[1, k : k + 1, :]
                mid_ref[k, rows, 0:HIGH] = pair[0] * cosine - pair[1] * sine
                mid_ref[k, rows, HIGH:] = pair[0] * sine + pair[1] * cosine

            low_transform(load, store, part_ref.at[g], -1)

    @pl.when(step >= WIDTH_STEPS)
    def _():
        base = (step - WIDTH_STEPS) * WIDTH_LOWS
        for k in range(WIDTH_LOWS):
            done = product(mid_ref[base + k], (high_ref, low_ref))
            for c in range(2):
                flat = done[:, HIGH * c : HIGH * (c + 1)].T
                for out_ref, start, count in zip(out_refs, STARTS, CHUNKS):
                    out_ref[k, c] = flat[start : start + count]


def whole(*dims):
    return pl.BlockSpec(dims, lambda i: (0,) * len(dims))


def along_width(target):
    high, low = block_table(-1.0, 1.0 / 64)
    shapes = [jax.ShapeDtypeStruct((LOW, 2, count, HIGH), jnp.float32) for count in CHUNKS]
    specs = [
        pl.BlockSpec(
            (WIDTH_LOWS, 2, count, HIGH), lambda i: (jnp.maximum(i - WIDTH_STEPS, 0), 0, 0, 0)
        )
        for count in CHUNKS
    ]
    return pl.pallas_call(
        width_kernel,
        name="along_width",
        grid=(2 * WIDTH_STEPS,),
        in_specs=[
            pl.BlockSpec(
                (1, 2, WIDTH_ROWS, N), lambda i: (0, 0, jnp.minimum(i, WIDTH_STEPS - 1), 0)
            ),
            whole(2, LOW, HIGH),
            whole(2 * HIGH, 2 * HIGH),
            whole(2 * HIGH, 2 * HIGH),
        ],
        out_specs=specs,
        out_shape=shapes,
        scratch_shapes=[
            pltpu.VMEM((LOW, HIGH, 2 * HIGH), jnp.float32),
            pltpu.VMEM((WIDTH_ROWS // 8, LOW, 2, 8, HIGH), jnp.float32),
        ],
        cost_estimate=pl.CostEstimate(
            flops=6 * N * 512 * 256, bytes_accessed=8 << 20, transcendentals=0
        ),
    )(target, jnp.asarray(twiddles(-1.0)), jnp.asarray(high), jnp.asarray(low))


HEIGHT_ROWS = 16


def height_kernel(x_ref, h_ref, ftw_ref, fh_ref, fl_ref, btw_ref, bh_ref, bl_ref,
                  out_ref, mid_ref, part_ref):
    groups = HEIGHT_ROWS // 8
    for g in range(groups):
        rows = slice(8 * g, 8 * g + 8)

        def load(n):
            return (x_ref[n, 0, rows, :], x_ref[n, 1, rows, :])

        def store(k, pair):
            cosine, sine = ftw_ref[0, k : k + 1, :], ftw_ref[1, k : k + 1, :]
            mid_ref[k, rows, 0:HIGH] = pair[0] * cosine - pair[1] * sine
            mid_ref[k, rows, HIGH:] = pair[0] * sine + pair[1] * cosine

        low_transform(load, store, part_ref.at[g], -1)

    count = 8
    for b in range(0, LOW, count):
        part = slice(b, b + count)
        flat = mid_ref[part].reshape(count * HEIGHT_ROWS, 2 * HIGH)
        spectrum = product(flat, (fh_ref, fl_ref))
        real, imaginary = spectrum[:, :HIGH], spectrum[:, HIGH:]
        cosine = h_ref[part, 0].reshape(count * HEIGHT_ROWS, HIGH)
        sine = h_ref[part, 1].reshape(count * HEIGHT_ROWS, HIGH)
        moved = jnp.concatenate(
            [real * cosine - imaginary * sine, real * sine + imaginary * cosine], axis=1
        )
        back = product(moved, (bh_ref, bl_ref))
        mid_ref[part] = back.reshape(count, HEIGHT_ROWS, 2 * HIGH)

    for g in range(groups):
        rows = slice(8 * g, 8 * g + 8)

        def load(k):
            real, imaginary = mid_ref[k, rows, 0:HIGH], mid_ref[k, rows, HIGH:]
            cosine, sine = btw_ref[0, k : k + 1, :], btw_ref[1, k : k + 1, :]
            return (real * cosine - imaginary * sine, real * sine + imaginary * cosine)

        def store(n, pair):
            out_ref[n, 0, rows, :] = pair[0]
            out_ref[n, 1, rows, :] = pair[1]

        low_transform(load, store, part_ref.at[g], 1)


def along_height(columns, transfer):
    spec = pl.BlockSpec((LOW, 2, HEIGHT_ROWS, HIGH), lambda i: (0, 0, i, 0))
    table = whole(2 * HIGH, 2 * HIGH)
    forward, backward = block_table(-1.0, 1.0 / 64), block_table(1.0, 1.0 / 64)
    count = columns.shape[2]
    return pl.pallas_call(
        height_kernel,
        name="along_height",
        grid=(count // HEIGHT_ROWS,),
        in_specs=[spec, spec, whole(2, LOW, HIGH), table, table, whole(2, LOW, HIGH), table, table],
        out_specs=spec,
        out_shape=jax.ShapeDtypeStruct((LOW, 2, count, HIGH), jnp.float32),
        scratch_shapes=[
            pltpu.VMEM((LOW, HEIGHT_ROWS, 2 * HIGH), jnp.float32),
            pltpu.VMEM((HEIGHT_ROWS // 8, LOW, 2, 8, HIGH), jnp.float32),
        ],
        cost_estimate=pl.CostEstimate(
            flops=12 * LOW * count * 512 * 256,
            bytes_accessed=3 * 8 * LOW * count * HIGH,
            transcendentals=0,
        ),
    )(
        columns,
        transfer,
        jnp.asarray(twiddles(-1.0)),
        *[jnp.asarray(t) for t in forward],
        jnp.asarray(twiddles(1.0)),
        *[jnp.asarray(t) for t in backward],
    )


def flip_kernel(share_ref, parts_ref, out_ref):
    for n in range(4):
        for c in range(2):
            total = parts_ref[n, c]
            for source in range(1, 8):
                total = total + parts_ref[4 * source + n, c]
            tile = jnp.concatenate([share_ref[n, c], total], axis=0)
            out_ref[16 * n : 16 * n + 16, c] = tile.T.reshape(16, 8, HIGH)


def flip(share, parts):
    return pl.pallas_call(
        flip_kernel,
        name="flip",
        out_shape=jax.ShapeDtypeStruct((64, 2, 8, HIGH), jnp.float32),
    )(share, parts)


def inverse_width_kernel(x_ref, tw_ref, high_ref, low_ref, out_ref, mid_ref, part_ref):
    total = x_ref[0:LOW] + x_ref[LOW:]
    rows = jnp.concatenate([total[:, 0], total[:, 1]], axis=-1).reshape(LOW * 8, 2 * HIGH)
    mid_ref[...] = product(rows, (high_ref, low_ref)).reshape(LOW, 8, 2 * HIGH)

    def load(k):
        real, imaginary = mid_ref[k, :, 0:HIGH], mid_ref[k, :, HIGH:]
        cosine, sine = tw_ref[0, k : k + 1, :], tw_ref[1, k : k + 1, :]
        return (real * cosine - imaginary * sine, real * sine + imaginary * cosine)

    def store(n, pair):
        out_ref[0, :, HIGH * n : HIGH * (n + 1)] = pair[0]
        out_ref[1, :, HIGH * n : HIGH * (n + 1)] = pair[1]

    low_transform(load, store, part_ref, 1)


def inverse_width(pieces, scaling):
    high, low = block_table(1.0, scaling / 64)
    return pl.pallas_call(
        inverse_width_kernel,
        name="inverse_width",
        out_shape=jax.ShapeDtypeStruct((2, 8, N), jnp.float32),
        scratch_shapes=[
            pltpu.VMEM((LOW, 8, 2 * HIGH), jnp.float32),
            pltpu.VMEM((LOW, 2, 8, HIGH), jnp.float32),
        ],
    )(pieces, jnp.asarray(twiddles(1.0)), jnp.asarray(high), jnp.asarray(low))


def signed(natural):
    return jnp.where(natural < N // 2, natural, natural - N)


def transfer_factors(depth_index, band_mask, column, start, count):
    high = jnp.arange(HIGH, dtype=jnp.int32)
    low = jnp.arange(LOW, dtype=jnp.int32)
    height = signed(low[:, None] + LOW * high[None, :])
    width = signed(column + LOW * (start + jnp.arange(count, dtype=jnp.int32)))
    square = (height * height)[:, None, :] + (width * width)[None, :, None]
    square = square.astype(jnp.float32) * np.float32(1.0 / (N * N))
    descent = -square / (jnp.sqrt(4.0 - square) + 2.0)
    turns = (100.0 + 2.0 * depth_index[0].astype(jnp.float32)) * descent
    angles = np.float32(2.0 * math.pi) * (turns - jnp.round(turns))
    mask_height = band_mask[0, 0].reshape(HIGH, LOW).T.astype(jnp.float32)
    mask_width = lax.dynamic_slice_in_dim(
        band_mask[0, 1].reshape(HIGH, LOW).T, column, 1, 0
    )[0, start : start + count].astype(jnp.float32)
    weights = mask_height[:, None, :] * mask_width[None, :, None]
    return jnp.stack([jnp.cos(angles) * weights, jnp.sin(angles) * weights], axis=1)


def hologram(target, depth_index, band_mask):
    spectra = along_width(target)
    transfer = [
        transfer_factors(depth_index, band_mask, lax.axis_index("rows"), start, count)
        for start, count in zip(STARTS, CHUNKS)
    ]
    parts = []
    for i, (block, start, count) in enumerate(zip(spectra, STARTS, CHUNKS)):
        columns = lax.all_to_all(block, "rows", split_axis=0, concat_axis=0, tiled=True)
        parts.append(along_height(columns, transfer[i]))
    share = lax.psum_scatter(parts[0], "depth_0", scatter_dimension=0, tiled=True)
    rest = lax.all_to_all(parts[1], "depth_0", split_axis=0, concat_axis=0, tiled=True)
    pieces = lax.all_to_all(
        flip(share, rest), ("depth_1", "rows"), split_axis=0, concat_axis=0, tiled=True
    )
    return inverse_width(pieces, 1.0 / math.sqrt(lax.axis_size(DEPTH)))


def solution(mesh):
    split = Mesh(mesh.devices.reshape(8, 2, mesh.shape["rows"]), ("depth_0", "depth_1", "rows"))
    in_specs = (P(DEPTH, None, "rows", None), P(DEPTH), P(DEPTH, None, None))
    out_specs = P(None, DEPTH_ROWS, None)
    return jax.shard_map(hologram, mesh=split, in_specs=in_specs, out_specs=out_specs, check_vma=False)
```

```python
import functools
import math

import jax
import jax.numpy as jnp
import numpy as np
from jax import lax
from jax.experimental import pallas as pl
from jax.experimental.pallas import tpu as pltpu
from jax.sharding import Mesh
from jax.sharding import PartitionSpec as P

LOW = 32
HIGH = 128
N = 4096
DEPTH = ("depth_0", "depth_1")
DEPTH_ROWS = ("depth_0", "depth_1", "rows")
CHUNKS = (64, 64)
STARTS = (0, 64)
PARTS = ((64,), (32, 32))


def block_table(direction, scaling):
    index = np.arange(HIGH)
    angles = direction * 2.0 * np.pi / HIGH * (index[:, None] * index[None, :] % HIGH)
    cosine, sine = np.cos(angles) * scaling, np.sin(angles) * scaling
    table = np.concatenate(
        [np.concatenate([cosine, sine], 1), np.concatenate([-sine, cosine], 1)], 0
    ).astype(np.float32)
    high = table.astype(jnp.bfloat16)
    low = (table - high.astype(np.float32)).astype(jnp.bfloat16)
    return high, low


def twiddles(direction):
    product = np.arange(LOW)[:, None] * np.arange(HIGH)[None, :] % N
    angles = direction * 2.0 * np.pi / N * product
    return np.stack([np.cos(angles), np.sin(angles)]).astype(np.float32)


def add(a, b):
    return (a[0] + b[0], a[1] + b[1])


def sub(a, b):
    return (a[0] - b[0], a[1] - b[1])


def quarter(a, sign):
    return (-a[1], a[0]) if sign > 0 else (a[1], -a[0])


def turn(a, numerator, length, sign):
    numerator %= length
    if numerator == 0:
        return a
    if numerator * 4 == length:
        return quarter(a, sign)
    if numerator * 2 == length:
        return (-a[0], -a[1])
    if numerator * 8 == length:
        half = np.float32(math.sqrt(0.5))
        b = quarter(a, sign)
        return ((a[0] + b[0]) * half, (a[1] + b[1]) * half)
    if numerator * 8 == 3 * length:
        half = np.float32(math.sqrt(0.5))
        b = quarter(a, sign)
        return ((b[0] - a[0]) * half, (b[1] - a[1]) * half)
    angle = sign * 2.0 * math.pi * numerator / length
    cosine, sine = np.float32(math.cos(angle)), np.float32(math.sin(angle))
    return (a[0] * cosine - a[1] * sine, a[0] * sine + a[1] * cosine)


def four_points(values, sign):
    even, odd = add(values[0], values[2]), sub(values[0], values[2])
    even_2, odd_2 = add(values[1], values[3]), quarter(sub(values[1], values[3]), sign)
    return [add(even, even_2), add(odd, odd_2), sub(even, even_2), sub(odd, odd_2)]


def eight_points(values, sign):
    first = four_points(values[0::2], sign)
    second = four_points(values[1::2], sign)
    second = [turn(second[k], k, 8, sign) for k in range(4)]
    return [add(first[k], second[k]) for k in range(4)] + [
        sub(first[k], second[k]) for k in range(4)
    ]


def low_transform(load, store, part_ref, sign):
    for a in range(8):
        outs = four_points([load(a + 8 * b) for b in range(4)], sign)
        for q in range(4):
            pair = turn(outs[q], a * q, 32, sign)
            part_ref[q * 8 + a, 0] = pair[0]
            part_ref[q * 8 + a, 1] = pair[1]
    for q in range(4):
        values = [(part_ref[q * 8 + a, 0], part_ref[q * 8 + a, 1]) for a in range(8)]
        outs = eight_points(values, sign)
        for p in range(8):
            store(q + 4 * p, outs[p])


def product(rows, table):
    high_table, low_table = table[0][...], table[1][...]
    high = rows.astype(jnp.bfloat16)
    low = (rows - high.astype(jnp.float32)).astype(jnp.bfloat16)
    dot = functools.partial(jnp.dot, preferred_element_type=jnp.float32)
    return dot(high, high_table) + (dot(low, high_table) + dot(high, low_table))


WIDTH_ROWS = 32
WIDTH_STEPS = HIGH // WIDTH_ROWS
WIDTH_LOWS = LOW // WIDTH_STEPS


def width_kernel(x_ref, tw_ref, high_ref, low_ref, *rest):
    out_refs, (mid_ref, part_ref) = rest[: len(CHUNKS)], rest[len(CHUNKS) :]
    step = pl.program_id(0)

    @pl.when(step < WIDTH_STEPS)
    def _():
        for g in range(WIDTH_ROWS // 8):
            rows = pl.ds(pl.multiple_of(step * WIDTH_ROWS + 8 * g, 8), 8)

            def load(n):
                lanes = slice(HIGH * n, HIGH * (n + 1))
                return (
                    x_ref[0, 0, 8 * g : 8 * g + 8, lanes],
                    x_ref[0, 1, 8 * g : 8 * g + 8, lanes],
                )

            def store(k, pair):
                cosine, sine = tw_ref[0, k : k + 1, :], tw_ref[1, k : k + 1, :]
                mid_ref[k, rows, 0:HIGH] = pair[0] * cosine - pair[1] * sine
                mid_ref[k, rows, HIGH:] = pair[0] * sine + pair[1] * cosine

            low_transform(load, store, part_ref.at[g], -1)

    @pl.when(step >= WIDTH_STEPS)
    def _():
        base = (step - WIDTH_STEPS) * WIDTH_LOWS
        for k in range(WIDTH_LOWS):
            done = product(mid_ref[base + k], (high_ref, low_ref))
            for c in range(2):
                flat = done[:, HIGH * c : HIGH * (c + 1)].T
                for out_ref, start, count in zip(out_refs, STARTS, CHUNKS):
                    out_ref[k, c] = flat[start : start + count]


def whole(*dims):
    return pl.BlockSpec(dims, lambda i: (0,) * len(dims))


def along_width(target):
    high, low = block_table(-1.0, 1.0 / 64)
    shapes = [jax.ShapeDtypeStruct((LOW, 2, count, HIGH), jnp.float32) for count in CHUNKS]
    specs = [
        pl.BlockSpec(
            (WIDTH_LOWS, 2, count, HIGH), lambda i: (jnp.maximum(i - WIDTH_STEPS, 0), 0, 0, 0)
        )
        for count in CHUNKS
    ]
    return pl.pallas_call(
        width_kernel,
        name="along_width",
        grid=(2 * WIDTH_STEPS,),
        in_specs=[
            pl.BlockSpec(
                (1, 2, WIDTH_ROWS, N), lambda i: (0, 0, jnp.minimum(i, WIDTH_STEPS - 1), 0)
            ),
            whole(2, LOW, HIGH),
            whole(2 * HIGH, 2 * HIGH),
            whole(2 * HIGH, 2 * HIGH),
        ],
        out_specs=specs,
        out_shape=shapes,
        scratch_shapes=[
            pltpu.VMEM((LOW, HIGH, 2 * HIGH), jnp.float32),
            pltpu.VMEM((WIDTH_ROWS // 8, LOW, 2, 8, HIGH), jnp.float32),
        ],
        cost_estimate=pl.CostEstimate(
            flops=6 * N * 512 * 256, bytes_accessed=8 << 20, transcendentals=0
        ),
    )(target, jnp.asarray(twiddles(-1.0)), jnp.asarray(high), jnp.asarray(low))


HEIGHT_ROWS = 16


def height_kernel(x_ref, h_ref, ftw_ref, fh_ref, fl_ref, btw_ref, bh_ref, bl_ref,
                  out_ref, mid_ref, part_ref):
    groups = HEIGHT_ROWS // 8
    for g in range(groups):
        rows = slice(8 * g, 8 * g + 8)

        def load(n):
            return (x_ref[n, 0, rows, :], x_ref[n, 1, rows, :])

        def store(k, pair):
            cosine, sine = ftw_ref[0, k : k + 1, :], ftw_ref[1, k : k + 1, :]
            mid_ref[k, rows, 0:HIGH] = pair[0] * cosine - pair[1] * sine
            mid_ref[k, rows, HIGH:] = pair[0] * sine + pair[1] * cosine

        low_transform(load, store, part_ref.at[g], -1)

    count = 8
    for b in range(0, LOW, count):
        part = slice(b, b + count)
        flat = mid_ref[part].reshape(count * HEIGHT_ROWS, 2 * HIGH)
        spectrum = product(flat, (fh_ref, fl_ref))
        real, imaginary = spectrum[:, :HIGH], spectrum[:, HIGH:]
        cosine = h_ref[part, 0].reshape(count * HEIGHT_ROWS, HIGH)
        sine = h_ref[part, 1].reshape(count * HEIGHT_ROWS, HIGH)
        moved = jnp.concatenate(
            [real * cosine - imaginary * sine, real * sine + imaginary * cosine], axis=1
        )
        back = product(moved, (bh_ref, bl_ref))
        mid_ref[part] = back.reshape(count, HEIGHT_ROWS, 2 * HIGH)

    for g in range(groups):
        rows = slice(8 * g, 8 * g + 8)

        def load(k):
            real, imaginary = mid_ref[k, rows, 0:HIGH], mid_ref[k, rows, HIGH:]
            cosine, sine = btw_ref[0, k : k + 1, :], btw_ref[1, k : k + 1, :]
            return (real * cosine - imaginary * sine, real * sine + imaginary * cosine)

        def store(n, pair):
            out_ref[n, 0, rows, :] = pair[0]
            out_ref[n, 1, rows, :] = pair[1]

        low_transform(load, store, part_ref.at[g], 1)


def along_height(columns, transfer, start, count):
    first = start // HEIGHT_ROWS
    block = (LOW, 2, HEIGHT_ROWS, HIGH)
    spec = pl.BlockSpec(block, lambda i: (0, 0, i, 0))
    moved = pl.BlockSpec(block, lambda i: (0, 0, i + first, 0))
    table = whole(2 * HIGH, 2 * HIGH)
    forward, backward = block_table(-1.0, 1.0 / 64), block_table(1.0, 1.0 / 64)
    return pl.pallas_call(
        height_kernel,
        name="along_height",
        grid=(count // HEIGHT_ROWS,),
        in_specs=[moved, moved, whole(2, LOW, HIGH), table, table, whole(2, LOW, HIGH), table, table],
        out_specs=spec,
        out_shape=jax.ShapeDtypeStruct((LOW, 2, count, HIGH), jnp.float32),
        scratch_shapes=[
            pltpu.VMEM((LOW, HEIGHT_ROWS, 2 * HIGH), jnp.float32),
            pltpu.VMEM((HEIGHT_ROWS // 8, LOW, 2, 8, HIGH), jnp.float32),
        ],
        cost_estimate=pl.CostEstimate(
            flops=12 * LOW * count * 512 * 256,
            bytes_accessed=3 * 8 * LOW * count * HIGH,
            transcendentals=0,
        ),
    )(
        columns,
        transfer,
        jnp.asarray(twiddles(-1.0)),
        *[jnp.asarray(t) for t in forward],
        jnp.asarray(twiddles(1.0)),
        *[jnp.asarray(t) for t in backward],
    )


def flip_kernel(*refs):
    in_refs, out_ref = refs[:-1], refs[-1]
    for c in range(2):
        tiles = []
        for ref in in_refs:
            total = ref[0, 0, c]
            for source in range(1, ref.shape[0]):
                total = total + ref[source, 0, c]
            tiles.append(total)
        out_ref[:, c] = jnp.concatenate(tiles, axis=0).T.reshape(16, 8, HIGH)


def flip(parts):
    return pl.pallas_call(
        flip_kernel,
        name="flip",
        grid=(4,),
        in_specs=[
            pl.BlockSpec((part.shape[0], 1) + part.shape[2:], lambda i: (0, i, 0, 0, 0))
            for part in parts
        ],
        out_specs=pl.BlockSpec((16, 2, 8, HIGH), lambda i: (i, 0, 0, 0)),
        out_shape=jax.ShapeDtypeStruct((64, 2, 8, HIGH), jnp.float32),
    )(*parts)


def inverse_width_kernel(x_ref, tw_ref, high_ref, low_ref, out_ref, mid_ref, part_ref):
    total = x_ref[0:LOW] + x_ref[LOW:]
    rows = jnp.concatenate([total[:, 0], total[:, 1]], axis=-1).reshape(LOW * 8, 2 * HIGH)
    mid_ref[...] = product(rows, (high_ref, low_ref)).reshape(LOW, 8, 2 * HIGH)

    def load(k):
        real, imaginary = mid_ref[k, :, 0:HIGH], mid_ref[k, :, HIGH:]
        cosine, sine = tw_ref[0, k : k + 1, :], tw_ref[1, k : k + 1, :]
        return (real * cosine - imaginary * sine, real * sine + imaginary * cosine)

    def store(n, pair):
        out_ref[0, :, HIGH * n : HIGH * (n + 1)] = pair[0]
        out_ref[1, :, HIGH * n : HIGH * (n + 1)] = pair[1]

    low_transform(load, store, part_ref, 1)


def inverse_width(pieces, scaling):
    high, low = block_table(1.0, scaling / 64)
    return pl.pallas_call(
        inverse_width_kernel,
        name="inverse_width",
        out_shape=jax.ShapeDtypeStruct((2, 8, N), jnp.float32),
        scratch_shapes=[
            pltpu.VMEM((LOW, 8, 2 * HIGH), jnp.float32),
            pltpu.VMEM((LOW, 2, 8, HIGH), jnp.float32),
        ],
    )(pieces, jnp.asarray(twiddles(1.0)), jnp.asarray(high), jnp.asarray(low))


def signed(natural):
    return jnp.where(natural < N // 2, natural, natural - N)


def transfer_factors(depth_index, band_mask, column, start, count):
    high = jnp.arange(HIGH, dtype=jnp.int32)
    low = jnp.arange(LOW, dtype=jnp.int32)
    height = signed(low[:, None] + LOW * high[None, :])
    width = signed(column + LOW * (start + jnp.arange(count, dtype=jnp.int32)))
    square = (height * height)[:, None, :] + (width * width)[None, :, None]
    square = square.astype(jnp.float32) * np.float32(1.0 / (N * N))
    descent = -square / (jnp.sqrt(4.0 - square) + 2.0)
    turns = (100.0 + 2.0 * depth_index[0].astype(jnp.float32)) * descent
    angles = np.float32(2.0 * math.pi) * (turns - jnp.round(turns))
    mask_height = band_mask[0, 0].reshape(HIGH, LOW).T.astype(jnp.float32)
    mask_width = lax.dynamic_slice_in_dim(
        band_mask[0, 1].reshape(HIGH, LOW).T, column, 1, 0
    )[0, start : start + count].astype(jnp.float32)
    weights = mask_height[:, None, :] * mask_width[None, :, None]
    return jnp.stack([jnp.cos(angles) * weights, jnp.sin(angles) * weights], axis=1)


def hologram(target, depth_index, band_mask):
    spectra = along_width(target)
    transfer = []
    for start, count in zip(STARTS, CHUNKS):
        column = lax.axis_index("rows")
        transfer.append(transfer_factors(depth_index, band_mask, column, start, count))
    shares = []
    for i, block in enumerate(spectra):
        columns = lax.all_to_all(block, "rows", split_axis=0, concat_axis=0, tiled=True)
        start = 0
        for j, count in enumerate(PARTS[i]):
            part = along_height(columns, transfer[i], start, count)
            start += count
            if j == 0:
                share = lax.psum_scatter(part, "depth_0", scatter_dimension=0, tiled=True)
                shares.append(share[None])
            else:
                share = lax.all_to_all(part, "depth_0", split_axis=0, concat_axis=0, tiled=True)
                shares.append(share.reshape(8, 4, 2, count, HIGH))
    pieces = lax.all_to_all(
        flip(shares), ("depth_1", "rows"), split_axis=0, concat_axis=0, tiled=True
    )
    return inverse_width(pieces, 1.0 / math.sqrt(lax.axis_size(DEPTH)))


def solution(mesh):
    split = Mesh(mesh.devices.reshape(8, 2, mesh.shape["rows"]), ("depth_0", "depth_1", "rows"))
    in_specs = (P(DEPTH, None, "rows", None), P(DEPTH), P(DEPTH, None, None))
    out_specs = P(None, DEPTH_ROWS, None)
    return jax.shard_map(hologram, mesh=split, in_specs=in_specs, out_specs=out_specs, check_vma=False)
```

```python
import functools
import math

import jax
import jax.numpy as jnp
import numpy as np
from jax import lax
from jax.experimental import pallas as pl
from jax.experimental.pallas import tpu as pltpu
from jax.sharding import Mesh
from jax.sharding import PartitionSpec as P

LOW = 32
HIGH = 128
N = 4096
DEPTH = ("depth_0", "depth_1")
DEPTH_ROWS = ("depth_0", "depth_1", "rows")
CHUNKS = (64, 64)
STARTS = (0, 64)


def block_table(direction, scaling):
    index = np.arange(HIGH)
    angles = direction * 2.0 * np.pi / HIGH * (index[:, None] * index[None, :] % HIGH)
    cosine, sine = np.cos(angles) * scaling, np.sin(angles) * scaling
    table = np.concatenate(
        [np.concatenate([cosine, sine], 1), np.concatenate([-sine, cosine], 1)], 0
    ).astype(np.float32)
    high = table.astype(jnp.bfloat16)
    low = (table - high.astype(np.float32)).astype(jnp.bfloat16)
    return high, low


def twiddles(direction):
    product = np.arange(LOW)[:, None] * np.arange(HIGH)[None, :] % N
    angles = direction * 2.0 * np.pi / N * product
    return np.stack([np.cos(angles), np.sin(angles)]).astype(np.float32)


def add(a, b):
    return (a[0] + b[0], a[1] + b[1])


def sub(a, b):
    return (a[0] - b[0], a[1] - b[1])


def quarter(a, sign):
    return (-a[1], a[0]) if sign > 0 else (a[1], -a[0])


def turn(a, numerator, length, sign):
    numerator %= length
    if numerator == 0:
        return a
    if numerator * 4 == length:
        return quarter(a, sign)
    if numerator * 2 == length:
        return (-a[0], -a[1])
    if numerator * 8 == length:
        half = np.float32(math.sqrt(0.5))
        b = quarter(a, sign)
        return ((a[0] + b[0]) * half, (a[1] + b[1]) * half)
    if numerator * 8 == 3 * length:
        half = np.float32(math.sqrt(0.5))
        b = quarter(a, sign)
        return ((b[0] - a[0]) * half, (b[1] - a[1]) * half)
    angle = sign * 2.0 * math.pi * numerator / length
    cosine, sine = np.float32(math.cos(angle)), np.float32(math.sin(angle))
    return (a[0] * cosine - a[1] * sine, a[0] * sine + a[1] * cosine)


def four_points(values, sign):
    even, odd = add(values[0], values[2]), sub(values[0], values[2])
    even_2, odd_2 = add(values[1], values[3]), quarter(sub(values[1], values[3]), sign)
    return [add(even, even_2), add(odd, odd_2), sub(even, even_2), sub(odd, odd_2)]


def eight_points(values, sign):
    first = four_points(values[0::2], sign)
    second = four_points(values[1::2], sign)
    second = [turn(second[k], k, 8, sign) for k in range(4)]
    return [add(first[k], second[k]) for k in range(4)] + [
        sub(first[k], second[k]) for k in range(4)
    ]


def low_transform(load, store, part_ref, sign):
    for a in range(8):
        outs = four_points([load(a + 8 * b) for b in range(4)], sign)
        for q in range(4):
            pair = turn(outs[q], a * q, 32, sign)
            part_ref[q * 8 + a, 0] = pair[0]
            part_ref[q * 8 + a, 1] = pair[1]
    for q in range(4):
        values = [(part_ref[q * 8 + a, 0], part_ref[q * 8 + a, 1]) for a in range(8)]
        outs = eight_points(values, sign)
        for p in range(8):
            store(q + 4 * p, outs[p])


def product(rows, table):
    high_table, low_table = table[0][...], table[1][...]
    high = rows.astype(jnp.bfloat16)
    low = (rows - high.astype(jnp.float32)).astype(jnp.bfloat16)
    dot = functools.partial(jnp.dot, preferred_element_type=jnp.float32)
    return dot(high, high_table) + (dot(low, high_table) + dot(high, low_table))


WIDTH_ROWS = 32
WIDTH_STEPS = HIGH // WIDTH_ROWS
WIDTH_LOWS = LOW // WIDTH_STEPS


def width_kernel(x_ref, tw_ref, high_ref, low_ref, *rest):
    out_refs, (mid_ref, part_ref) = rest[: len(CHUNKS)], rest[len(CHUNKS) :]
    step = pl.program_id(0)

    @pl.when(step < WIDTH_STEPS)
    def _():
        for g in range(WIDTH_ROWS // 8):
            rows = pl.ds(pl.multiple_of(step * WIDTH_ROWS + 8 * g, 8), 8)

            def load(n):
                lanes = slice(HIGH * n, HIGH * (n + 1))
                return (
                    x_ref[0, 0, 8 * g : 8 * g + 8, lanes],
                    x_ref[0, 1, 8 * g : 8 * g + 8, lanes],
                )

            def store(k, pair):
                cosine, sine = tw_ref[0, k : k + 1, :], tw_ref[1, k : k + 1, :]
                mid_ref[k, rows, 0:HIGH] = pair[0] * cosine - pair[1] * sine
                mid_ref[k, rows, HIGH:] = pair[0] * sine + pair[1] * cosine

            low_transform(load, store, part_ref.at[g], -1)

    @pl.when(step >= WIDTH_STEPS)
    def _():
        base = (step - WIDTH_STEPS) * WIDTH_LOWS
        for k in range(WIDTH_LOWS):
            done = product(mid_ref[base + k], (high_ref, low_ref))
            for c in range(2):
                flat = done[:, HIGH * c : HIGH * (c + 1)].T
                for out_ref, start, count in zip(out_refs, STARTS, CHUNKS):
                    out_ref[k, c] = flat[start : start + count]


def whole(*dims):
    return pl.BlockSpec(dims, lambda i: (0,) * len(dims))


def along_width(target):
    high, low = block_table(-1.0, 1.0 / 64)
    shapes = [jax.ShapeDtypeStruct((LOW, 2, count, HIGH), jnp.float32) for count in CHUNKS]
    specs = [
        pl.BlockSpec(
            (WIDTH_LOWS, 2, count, HIGH), lambda i: (jnp.maximum(i - WIDTH_STEPS, 0), 0, 0, 0)
        )
        for count in CHUNKS
    ]
    return pl.pallas_call(
        width_kernel,
        name="along_width",
        grid=(2 * WIDTH_STEPS,),
        in_specs=[
            pl.BlockSpec(
                (1, 2, WIDTH_ROWS, N), lambda i: (0, 0, jnp.minimum(i, WIDTH_STEPS - 1), 0)
            ),
            whole(2, LOW, HIGH),
            whole(2 * HIGH, 2 * HIGH),
            whole(2 * HIGH, 2 * HIGH),
        ],
        out_specs=specs,
        out_shape=shapes,
        scratch_shapes=[
            pltpu.VMEM((LOW, HIGH, 2 * HIGH), jnp.float32),
            pltpu.VMEM((WIDTH_ROWS // 8, LOW, 2, 8, HIGH), jnp.float32),
        ],
        cost_estimate=pl.CostEstimate(
            flops=6 * N * 512 * 256, bytes_accessed=8 << 20, transcendentals=0
        ),
    )(target, jnp.asarray(twiddles(-1.0)), jnp.asarray(high), jnp.asarray(low))


HEIGHT_ROWS = 16


def height_kernel(x_ref, h_ref, ftw_ref, fh_ref, fl_ref, btw_ref, bh_ref, bl_ref,
                  out_ref, mid_ref, part_ref):
    groups = HEIGHT_ROWS // 8
    for g in range(groups):
        rows = slice(8 * g, 8 * g + 8)

        def load(n):
            return (x_ref[n, 0, rows, :], x_ref[n, 1, rows, :])

        def store(k, pair):
            cosine, sine = ftw_ref[0, k : k + 1, :], ftw_ref[1, k : k + 1, :]
            mid_ref[k, rows, 0:HIGH] = pair[0] * cosine - pair[1] * sine
            mid_ref[k, rows, HIGH:] = pair[0] * sine + pair[1] * cosine

        low_transform(load, store, part_ref.at[g], -1)

    count = 8
    for b in range(0, LOW, count):
        part = slice(b, b + count)
        flat = mid_ref[part].reshape(count * HEIGHT_ROWS, 2 * HIGH)
        spectrum = product(flat, (fh_ref, fl_ref))
        real, imaginary = spectrum[:, :HIGH], spectrum[:, HIGH:]
        cosine = h_ref[part, 0].reshape(count * HEIGHT_ROWS, HIGH)
        sine = h_ref[part, 1].reshape(count * HEIGHT_ROWS, HIGH)
        moved = jnp.concatenate(
            [real * cosine - imaginary * sine, real * sine + imaginary * cosine], axis=1
        )
        back = product(moved, (bh_ref, bl_ref))
        mid_ref[part] = back.reshape(count, HEIGHT_ROWS, 2 * HIGH)

    for g in range(groups):
        rows = slice(8 * g, 8 * g + 8)

        def load(k):
            real, imaginary = mid_ref[k, rows, 0:HIGH], mid_ref[k, rows, HIGH:]
            cosine, sine = btw_ref[0, k : k + 1, :], btw_ref[1, k : k + 1, :]
            return (real * cosine - imaginary * sine, real * sine + imaginary * cosine)

        def store(n, pair):
            out_ref[n, 0, rows, :] = pair[0]
            out_ref[n, 1, rows, :] = pair[1]

        low_transform(load, store, part_ref.at[g], 1)


def along_height(columns, transfer):
    count = columns.shape[2]
    spec = pl.BlockSpec((LOW, 2, HEIGHT_ROWS, HIGH), lambda i: (0, 0, i, 0))
    table = whole(2 * HIGH, 2 * HIGH)
    forward, backward = block_table(-1.0, 1.0 / 64), block_table(1.0, 1.0 / 64)
    return pl.pallas_call(
        height_kernel,
        name="along_height",
        grid=(count // HEIGHT_ROWS,),
        in_specs=[spec, spec, whole(2, LOW, HIGH), table, table, whole(2, LOW, HIGH), table, table],
        out_specs=spec,
        out_shape=jax.ShapeDtypeStruct((LOW, 2, count, HIGH), jnp.float32),
        scratch_shapes=[
            pltpu.VMEM((LOW, HEIGHT_ROWS, 2 * HIGH), jnp.float32),
            pltpu.VMEM((HEIGHT_ROWS // 8, LOW, 2, 8, HIGH), jnp.float32),
        ],
        cost_estimate=pl.CostEstimate(
            flops=12 * LOW * count * 512 * 256,
            bytes_accessed=3 * 8 * LOW * count * HIGH,
            transcendentals=0,
        ),
    )(
        columns,
        transfer,
        jnp.asarray(twiddles(-1.0)),
        *[jnp.asarray(t) for t in forward],
        jnp.asarray(twiddles(1.0)),
        *[jnp.asarray(t) for t in backward],
    )


def flip_kernel(x_ref, out_ref):
    for n in range(4):
        tile = jnp.concatenate([x_ref[n, 0], x_ref[n, 1]], axis=0)
        out_ref[16 * n : 16 * n + 16] = tile.T.reshape(16, 8, HIGH)


def flip(share):
    return pl.pallas_call(
        flip_kernel,
        name="flip",
        out_shape=jax.ShapeDtypeStruct((64, 8, HIGH), jnp.float32),
        cost_estimate=pl.CostEstimate(flops=1 << 18, bytes_accessed=1 << 19, transcendentals=0),
    )(share)


def inverse_width_kernel(
    first_ref, second_ref, tw_ref, high_ref, low_ref, out_ref, mid_ref, part_ref
):
    rows = jnp.concatenate(
        [ref[0:LOW] + ref[LOW:] for ref in (first_ref, second_ref)], axis=-1
    ).reshape(LOW * 8, 2 * HIGH)
    mid_ref[...] = product(rows, (high_ref, low_ref)).reshape(LOW, 8, 2 * HIGH)

    def load(k):
        real, imaginary = mid_ref[k, :, 0:HIGH], mid_ref[k, :, HIGH:]
        cosine, sine = tw_ref[0, k : k + 1, :], tw_ref[1, k : k + 1, :]
        return (real * cosine - imaginary * sine, real * sine + imaginary * cosine)

    def store(n, pair):
        out_ref[0, :, HIGH * n : HIGH * (n + 1)] = pair[0]
        out_ref[1, :, HIGH * n : HIGH * (n + 1)] = pair[1]

    low_transform(load, store, part_ref, 1)


def inverse_width(pieces, scaling):
    high, low = [
        table.reshape(2, 2, HIGH // 2, 2 * HIGH).swapaxes(0, 1).reshape(table.shape)
        for table in block_table(1.0, scaling / 64)
    ]
    return pl.pallas_call(
        inverse_width_kernel,
        name="inverse_width",
        out_shape=jax.ShapeDtypeStruct((2, 8, N), jnp.float32),
        scratch_shapes=[
            pltpu.VMEM((LOW, 8, 2 * HIGH), jnp.float32),
            pltpu.VMEM((LOW, 2, 8, HIGH), jnp.float32),
        ],
    )(*pieces, jnp.asarray(twiddles(1.0)), jnp.asarray(high), jnp.asarray(low))


def signed(natural):
    return jnp.where(natural < N // 2, natural, natural - N)


def transfer_factors(depth_index, band_mask, column, start, count):
    high = jnp.arange(HIGH, dtype=jnp.int32)
    low = jnp.arange(LOW, dtype=jnp.int32)
    height = signed(low[:, None] + LOW * high[None, :])
    width = signed(column + LOW * (start + jnp.arange(count, dtype=jnp.int32)))
    square = (height * height)[:, None, :] + (width * width)[None, :, None]
    square = square.astype(jnp.float32) * np.float32(1.0 / (N * N))
    descent = -square / (jnp.sqrt(4.0 - square) + 2.0)
    turns = (100.0 + 2.0 * depth_index[0].astype(jnp.float32)) * descent
    angles = np.float32(2.0 * math.pi) * (turns - jnp.round(turns))
    mask_height = band_mask[0, 0].reshape(HIGH, LOW).T.astype(jnp.float32)
    mask_width = lax.dynamic_slice_in_dim(
        band_mask[0, 1].reshape(HIGH, LOW).T, column, 1, 0
    )[0, start : start + count].astype(jnp.float32)
    weights = mask_height[:, None, :] * mask_width[None, :, None]
    return jnp.stack([jnp.cos(angles) * weights, jnp.sin(angles) * weights], axis=1)


def hologram(target, depth_index, band_mask):
    spectra = along_width(target)
    transfer = []
    for start, count in zip(STARTS, CHUNKS):
        column = lax.axis_index("rows")
        transfer.append(transfer_factors(depth_index, band_mask, column, start, count))
    pieces = []
    for i, block in enumerate(spectra):
        columns = lax.all_to_all(block, "rows", split_axis=0, concat_axis=0, tiled=True)
        part = along_height(columns, transfer[i])
        share = lax.psum_scatter(part, "depth_0", scatter_dimension=0, tiled=True)
        pieces.append(
            lax.all_to_all(
                flip(share), ("depth_1", "rows"), split_axis=0, concat_axis=0, tiled=True
            )
        )
    return inverse_width(pieces, 1.0 / math.sqrt(lax.axis_size(DEPTH)))


def solution(mesh):
    split = Mesh(mesh.devices.reshape(8, 2, mesh.shape["rows"]), ("depth_0", "depth_1", "rows"))
    in_specs = (P(DEPTH, None, "rows", None), P(DEPTH), P(DEPTH, None, None))
    out_specs = P(None, DEPTH_ROWS, None)
    return jax.shard_map(hologram, mesh=split, in_specs=in_specs, out_specs=out_specs, check_vma=False)
```

```python
import functools
import math

import jax
import jax.numpy as jnp
import numpy as np
from jax import lax
from jax.experimental import pallas as pl
from jax.experimental.pallas import tpu as pltpu
from jax.sharding import Mesh
from jax.sharding import PartitionSpec as P

LOW = 32
HIGH = 128
N = 4096
DEPTH = ("depth_0", "depth_1")
DEPTH_ROWS = ("depth_0", "depth_1", "rows")
CHUNKS = (64, 64)
STARTS = (0, 64)


def block_table(direction, scaling):
    index = np.arange(HIGH)
    angles = direction * 2.0 * np.pi / HIGH * (index[:, None] * index[None, :] % HIGH)
    cosine, sine = np.cos(angles) * scaling, np.sin(angles) * scaling
    table = np.concatenate(
        [np.concatenate([cosine, sine], 1), np.concatenate([-sine, cosine], 1)], 0
    ).astype(np.float32)
    high = table.astype(jnp.bfloat16)
    low = (table - high.astype(np.float32)).astype(jnp.bfloat16)
    return high, low


def twiddles(direction):
    product = np.arange(LOW)[:, None] * np.arange(HIGH)[None, :] % N
    angles = direction * 2.0 * np.pi / N * product
    return np.stack([np.cos(angles), np.sin(angles)]).astype(np.float32)


def add(a, b):
    return (a[0] + b[0], a[1] + b[1])


def sub(a, b):
    return (a[0] - b[0], a[1] - b[1])


def quarter(a, sign):
    return (-a[1], a[0]) if sign > 0 else (a[1], -a[0])


def turn(a, numerator, length, sign):
    numerator %= length
    if numerator == 0:
        return a
    if numerator * 4 == length:
        return quarter(a, sign)
    if numerator * 2 == length:
        return (-a[0], -a[1])
    if numerator * 8 == length:
        half = np.float32(math.sqrt(0.5))
        b = quarter(a, sign)
        return ((a[0] + b[0]) * half, (a[1] + b[1]) * half)
    if numerator * 8 == 3 * length:
        half = np.float32(math.sqrt(0.5))
        b = quarter(a, sign)
        return ((b[0] - a[0]) * half, (b[1] - a[1]) * half)
    angle = sign * 2.0 * math.pi * numerator / length
    cosine, sine = np.float32(math.cos(angle)), np.float32(math.sin(angle))
    return (a[0] * cosine - a[1] * sine, a[0] * sine + a[1] * cosine)


def four_points(values, sign):
    even, odd = add(values[0], values[2]), sub(values[0], values[2])
    even_2, odd_2 = add(values[1], values[3]), quarter(sub(values[1], values[3]), sign)
    return [add(even, even_2), add(odd, odd_2), sub(even, even_2), sub(odd, odd_2)]


def eight_points(values, sign):
    first = four_points(values[0::2], sign)
    second = four_points(values[1::2], sign)
    second = [turn(second[k], k, 8, sign) for k in range(4)]
    return [add(first[k], second[k]) for k in range(4)] + [
        sub(first[k], second[k]) for k in range(4)
    ]


def low_transform(load, store, part_ref, sign):
    for a in range(8):
        outs = four_points([load(a + 8 * b) for b in range(4)], sign)
        for q in range(4):
            pair = turn(outs[q], a * q, 32, sign)
            part_ref[q * 8 + a, 0] = pair[0]
            part_ref[q * 8 + a, 1] = pair[1]
    for q in range(4):
        values = [(part_ref[q * 8 + a, 0], part_ref[q * 8 + a, 1]) for a in range(8)]
        outs = eight_points(values, sign)
        for p in range(8):
            store(q + 4 * p, outs[p])


def product(rows, table):
    high_table, low_table = table[0][...], table[1][...]
    high = rows.astype(jnp.bfloat16)
    low = (rows - high.astype(jnp.float32)).astype(jnp.bfloat16)
    dot = functools.partial(jnp.dot, preferred_element_type=jnp.float32)
    return dot(high, high_table) + (dot(low, high_table) + dot(high, low_table))


WIDTH_ROWS = 32
WIDTH_STEPS = HIGH // WIDTH_ROWS
WIDTH_LOWS = LOW // WIDTH_STEPS


def width_kernel(x_ref, tw_ref, high_ref, low_ref, out_ref, mid_ref, part_ref):
    step = pl.program_id(0)

    @pl.when(step < WIDTH_STEPS)
    def _():
        for g in range(WIDTH_ROWS // 8):
            rows = pl.ds(pl.multiple_of(step * WIDTH_ROWS + 8 * g, 8), 8)

            def load(n):
                lanes = slice(HIGH * n, HIGH * (n + 1))
                return (
                    x_ref[0, 0, 8 * g : 8 * g + 8, lanes],
                    x_ref[0, 1, 8 * g : 8 * g + 8, lanes],
                )

            def store(k, pair):
                cosine, sine = tw_ref[0, k : k + 1, :], tw_ref[1, k : k + 1, :]
                mid_ref[k, rows, 0:HIGH] = pair[0] * cosine - pair[1] * sine
                mid_ref[k, rows, HIGH:] = pair[0] * sine + pair[1] * cosine

            low_transform(load, store, part_ref.at[g], -1)

    @pl.when(step >= WIDTH_STEPS)
    def _():
        base = (step - WIDTH_STEPS) * WIDTH_LOWS
        for k in range(WIDTH_LOWS):
            flat = product(mid_ref[base + k], (high_ref, low_ref)).T
            out_ref[k, 0] = flat[: flat.shape[0] // 2]
            out_ref[k, 1] = flat[flat.shape[0] // 2 :]


def whole(*dims):
    return pl.BlockSpec(dims, lambda i: (0,) * len(dims))


def along_width(target, start, count):
    high, low = [
        np.concatenate(
            [table[:, start : start + count], table[:, HIGH + start : HIGH + start + count]], 1
        )
        for table in block_table(-1.0, 1.0 / 64)
    ]
    return pl.pallas_call(
        width_kernel,
        name="along_width",
        grid=(2 * WIDTH_STEPS,),
        in_specs=[
            pl.BlockSpec(
                (1, 2, WIDTH_ROWS, N), lambda i: (0, 0, jnp.minimum(i, WIDTH_STEPS - 1), 0)
            ),
            whole(2, LOW, HIGH),
            whole(2 * HIGH, 2 * count),
            whole(2 * HIGH, 2 * count),
        ],
        out_specs=pl.BlockSpec(
            (WIDTH_LOWS, 2, count, HIGH), lambda i: (jnp.maximum(i - WIDTH_STEPS, 0), 0, 0, 0)
        ),
        out_shape=jax.ShapeDtypeStruct((LOW, 2, count, HIGH), jnp.float32),
        scratch_shapes=[
            pltpu.VMEM((LOW, HIGH, 2 * HIGH), jnp.float32),
            pltpu.VMEM((WIDTH_ROWS // 8, LOW, 2, 8, HIGH), jnp.float32),
        ],
        cost_estimate=pl.CostEstimate(
            flops=6 * N * 512 * 2 * count, bytes_accessed=6 << 20, transcendentals=0
        ),
    )(target, jnp.asarray(twiddles(-1.0)), jnp.asarray(high), jnp.asarray(low))


HEIGHT_ROWS = 16


def height_kernel(x_ref, h_ref, ftw_ref, fh_ref, fl_ref, btw_ref, bh_ref, bl_ref,
                  out_ref, mid_ref, part_ref):
    groups = HEIGHT_ROWS // 8
    for g in range(groups):
        rows = slice(8 * g, 8 * g + 8)

        def load(n):
            return (x_ref[n, 0, rows, :], x_ref[n, 1, rows, :])

        def store(k, pair):
            cosine, sine = ftw_ref[0, k : k + 1, :], ftw_ref[1, k : k + 1, :]
            mid_ref[k, rows, 0:HIGH] = pair[0] * cosine - pair[1] * sine
            mid_ref[k, rows, HIGH:] = pair[0] * sine + pair[1] * cosine

        low_transform(load, store, part_ref.at[g], -1)

    count = 8
    for b in range(0, LOW, count):
        part = slice(b, b + count)
        flat = mid_ref[part].reshape(count * HEIGHT_ROWS, 2 * HIGH)
        spectrum = product(flat, (fh_ref, fl_ref))
        real, imaginary = spectrum[:, :HIGH], spectrum[:, HIGH:]
        cosine = h_ref[part, 0].reshape(count * HEIGHT_ROWS, HIGH)
        sine = h_ref[part, 1].reshape(count * HEIGHT_ROWS, HIGH)
        moved = jnp.concatenate(
            [real * cosine - imaginary * sine, real * sine + imaginary * cosine], axis=1
        )
        back = product(moved, (bh_ref, bl_ref))
        mid_ref[part] = back.reshape(count, HEIGHT_ROWS, 2 * HIGH)

    for g in range(groups):
        rows = slice(8 * g, 8 * g + 8)

        def load(k):
            real, imaginary = mid_ref[k, rows, 0:HIGH], mid_ref[k, rows, HIGH:]
            cosine, sine = btw_ref[0, k : k + 1, :], btw_ref[1, k : k + 1, :]
            return (real * cosine - imaginary * sine, real * sine + imaginary * cosine)

        def store(n, pair):
            out_ref[n, 0, rows, :] = pair[0]
            out_ref[n, 1, rows, :] = pair[1]

        low_transform(load, store, part_ref.at[g], 1)


def along_height(columns, transfer):
    count = columns.shape[2]
    spec = pl.BlockSpec((LOW, 2, HEIGHT_ROWS, HIGH), lambda i: (0, 0, i, 0))
    table = whole(2 * HIGH, 2 * HIGH)
    forward, backward = block_table(-1.0, 1.0 / 64), block_table(1.0, 1.0 / 64)
    return pl.pallas_call(
        height_kernel,
        name="along_height",
        compiler_params=pltpu.CompilerParams(vmem_limit_bytes=14 << 20),
        grid=(count // HEIGHT_ROWS,),
        in_specs=[spec, spec, whole(2, LOW, HIGH), table, table, whole(2, LOW, HIGH), table, table],
        out_specs=spec,
        out_shape=pltpu.HBM((LOW, 2, count, HIGH), jnp.float32),
        scratch_shapes=[
            pltpu.VMEM((LOW, HEIGHT_ROWS, 2 * HIGH), jnp.float32),
            pltpu.VMEM((HEIGHT_ROWS // 8, LOW, 2, 8, HIGH), jnp.float32),
        ],
        cost_estimate=pl.CostEstimate(
            flops=12 * LOW * count * 512 * 256,
            bytes_accessed=3 * 8 * LOW * count * HIGH,
            transcendentals=0,
        ),
    )(
        columns,
        transfer,
        jnp.asarray(twiddles(-1.0)),
        *[jnp.asarray(t) for t in forward],
        jnp.asarray(twiddles(1.0)),
        *[jnp.asarray(t) for t in backward],
    )


def flip_kernel(x_ref, out_ref):
    for n in range(4):
        tile = jnp.concatenate([x_ref[n, 0], x_ref[n, 1]], axis=0)
        out_ref[16 * n : 16 * n + 16] = tile.T.reshape(16, 8, HIGH)


def flip(share):
    return pl.pallas_call(
        flip_kernel,
        name="flip",
        out_shape=jax.ShapeDtypeStruct((64, 8, HIGH), jnp.float32),
        cost_estimate=pl.CostEstimate(flops=1 << 18, bytes_accessed=1 << 19, transcendentals=0),
    )(share)


def inverse_width_kernel(
    first_ref, second_ref, tw_ref, high_ref, low_ref, out_ref, mid_ref, part_ref
):
    rows = jnp.concatenate(
        [ref[0:LOW] + ref[LOW:] for ref in (first_ref, second_ref)], axis=-1
    ).reshape(LOW * 8, 2 * HIGH)
    mid_ref[...] = product(rows, (high_ref, low_ref)).reshape(LOW, 8, 2 * HIGH)

    def load(k):
        real, imaginary = mid_ref[k, :, 0:HIGH], mid_ref[k, :, HIGH:]
        cosine, sine = tw_ref[0, k : k + 1, :], tw_ref[1, k : k + 1, :]
        return (real * cosine - imaginary * sine, real * sine + imaginary * cosine)

    def store(n, pair):
        out_ref[0, :, HIGH * n : HIGH * (n + 1)] = pair[0]
        out_ref[1, :, HIGH * n : HIGH * (n + 1)] = pair[1]

    low_transform(load, store, part_ref, 1)


def inverse_width(pieces, scaling):
    high, low = [
        table.reshape(2, 2, HIGH // 2, 2 * HIGH).swapaxes(0, 1).reshape(table.shape)
        for table in block_table(1.0, scaling / 64)
    ]
    return pl.pallas_call(
        inverse_width_kernel,
        name="inverse_width",
        compiler_params=pltpu.CompilerParams(vmem_limit_bytes=8 << 20),
        out_shape=jax.ShapeDtypeStruct((2, 8, N), jnp.float32),
        scratch_shapes=[
            pltpu.VMEM((LOW, 8, 2 * HIGH), jnp.float32),
            pltpu.VMEM((LOW, 2, 8, HIGH), jnp.float32),
        ],
    )(*pieces, jnp.asarray(twiddles(1.0)), jnp.asarray(high), jnp.asarray(low))


def signed(natural):
    return jnp.where(natural < N // 2, natural, natural - N)


def transfer_factors(depth_index, band_mask, column, start, count):
    high = jnp.arange(HIGH, dtype=jnp.int32)
    low = jnp.arange(LOW, dtype=jnp.int32)
    height = signed(low[:, None] + LOW * high[None, :])
    width = signed(column + LOW * (start + jnp.arange(count, dtype=jnp.int32)))
    square = (height * height)[:, None, :] + (width * width)[None, :, None]
    square = square.astype(jnp.float32) * np.float32(1.0 / (N * N))
    descent = -square / (jnp.sqrt(4.0 - square) + 2.0)
    turns = (100.0 + 2.0 * depth_index[0].astype(jnp.float32)) * descent
    angles = np.float32(2.0 * math.pi) * (turns - jnp.round(turns))
    mask_height = band_mask[0, 0].reshape(HIGH, LOW).T.astype(jnp.float32)
    mask_width = lax.dynamic_slice_in_dim(
        band_mask[0, 1].reshape(HIGH, LOW).T, column, 1, 0
    )[0, start : start + count].astype(jnp.float32)
    weights = mask_height[:, None, :] * mask_width[None, :, None]
    return jnp.stack([jnp.cos(angles) * weights, jnp.sin(angles) * weights], axis=1)


def hologram(target, depth_index, band_mask):
    transfer = []
    for start, count in zip(STARTS, CHUNKS):
        column = lax.axis_index("rows")
        transfer.append(transfer_factors(depth_index, band_mask, column, start, count))
    pieces = []
    for i, (start, count) in enumerate(zip(STARTS, CHUNKS)):
        block = along_width(target, start, count)
        columns = lax.all_to_all(block, "rows", split_axis=0, concat_axis=0, tiled=True)
        part = along_height(columns, transfer[i])
        share = lax.psum_scatter(part, "depth_0", scatter_dimension=0, tiled=True)
        pieces.append(
            lax.all_to_all(
                flip(share), ("depth_1", "rows"), split_axis=0, concat_axis=0, tiled=True
            )
        )
    return inverse_width(pieces, 1.0 / math.sqrt(lax.axis_size(DEPTH)))


def solution(mesh):
    split = Mesh(mesh.devices.reshape(8, 2, mesh.shape["rows"]), ("depth_0", "depth_1", "rows"))
    in_specs = (P(DEPTH, None, "rows", None), P(DEPTH), P(DEPTH, None, None))
    out_specs = P(None, DEPTH_ROWS, None)
    return jax.shard_map(hologram, mesh=split, in_specs=in_specs, out_specs=out_specs, check_vma=False)
```

```python
import functools
import math

import jax
import jax.numpy as jnp
import numpy as np
from jax import lax
from jax.experimental import pallas as pl
from jax.experimental.pallas import tpu as pltpu
from jax.sharding import Mesh
from jax.sharding import PartitionSpec as P

LOW = 32
HIGH = 128
N = 4096
DEPTH = ("depth_0", "depth_1")
DEPTH_ROWS = ("depth_0", "depth_1", "rows")
CHUNKS = (64, 64)
STARTS = (0, 64)


def block_table(direction, scaling):
    index = np.arange(HIGH)
    angles = direction * 2.0 * np.pi / HIGH * (index[:, None] * index[None, :] % HIGH)
    cosine, sine = np.cos(angles) * scaling, np.sin(angles) * scaling
    table = np.concatenate(
        [np.concatenate([cosine, sine], 1), np.concatenate([-sine, cosine], 1)], 0
    ).astype(np.float32)
    high = table.astype(jnp.bfloat16)
    low = (table - high.astype(np.float32)).astype(jnp.bfloat16)
    return high, low


def twiddles(direction):
    product = np.arange(LOW)[:, None] * np.arange(HIGH)[None, :] % N
    angles = direction * 2.0 * np.pi / N * product
    return np.stack([np.cos(angles), np.sin(angles)]).astype(np.float32)


def add(a, b):
    return (a[0] + b[0], a[1] + b[1])


def sub(a, b):
    return (a[0] - b[0], a[1] - b[1])


def quarter(a, sign):
    return (-a[1], a[0]) if sign > 0 else (a[1], -a[0])


def turn(a, numerator, length, sign):
    numerator %= length
    if numerator == 0:
        return a
    if numerator * 4 == length:
        return quarter(a, sign)
    if numerator * 2 == length:
        return (-a[0], -a[1])
    if numerator * 8 == length:
        half = np.float32(math.sqrt(0.5))
        b = quarter(a, sign)
        return ((a[0] + b[0]) * half, (a[1] + b[1]) * half)
    if numerator * 8 == 3 * length:
        half = np.float32(math.sqrt(0.5))
        b = quarter(a, sign)
        return ((b[0] - a[0]) * half, (b[1] - a[1]) * half)
    angle = sign * 2.0 * math.pi * numerator / length
    cosine, sine = np.float32(math.cos(angle)), np.float32(math.sin(angle))
    return (a[0] * cosine - a[1] * sine, a[0] * sine + a[1] * cosine)


def four_points(values, sign):
    even, odd = add(values[0], values[2]), sub(values[0], values[2])
    even_2, odd_2 = add(values[1], values[3]), quarter(sub(values[1], values[3]), sign)
    return [add(even, even_2), add(odd, odd_2), sub(even, even_2), sub(odd, odd_2)]


def eight_points(values, sign):
    first = four_points(values[0::2], sign)
    second = four_points(values[1::2], sign)
    second = [turn(second[k], k, 8, sign) for k in range(4)]
    return [add(first[k], second[k]) for k in range(4)] + [
        sub(first[k], second[k]) for k in range(4)
    ]


def low_transform(load, store, part_ref, sign):
    for a in range(8):
        outs = four_points([load(a + 8 * b) for b in range(4)], sign)
        for q in range(4):
            pair = turn(outs[q], a * q, 32, sign)
            part_ref[q * 8 + a, 0] = pair[0]
            part_ref[q * 8 + a, 1] = pair[1]
    for q in range(4):
        values = [(part_ref[q * 8 + a, 0], part_ref[q * 8 + a, 1]) for a in range(8)]
        outs = eight_points(values, sign)
        for p in range(8):
            store(q + 4 * p, outs[p])


def product(rows, table):
    high_table, low_table = table[0][...], table[1][...]
    high = rows.astype(jnp.bfloat16)
    low = (rows - high.astype(jnp.float32)).astype(jnp.bfloat16)
    dot = functools.partial(jnp.dot, preferred_element_type=jnp.float32)
    return dot(high, high_table) + (dot(low, high_table) + dot(high, low_table))


WIDTH_ROWS = 32
WIDTH_STEPS = HIGH // WIDTH_ROWS
WIDTH_LOWS = LOW // WIDTH_STEPS


def narrow_product(rows, high_ref, both_ref):
    high = rows.astype(jnp.bfloat16)
    low = (rows - high.astype(jnp.float32)).astype(jnp.bfloat16)
    first = jnp.dot(high, both_ref[...], preferred_element_type=jnp.float32)
    second = jnp.dot(low, high_ref[...], preferred_element_type=jnp.float32)
    return first[:, :HIGH] + (first[:, HIGH:] + second)


def width_kernel(x_ref, tw_ref, high_ref, both_ref, out_ref, mid_ref, part_ref):
    step = pl.program_id(0)

    @pl.when(step < WIDTH_STEPS)
    def _():
        for g in range(WIDTH_ROWS // 8):
            rows = pl.ds(pl.multiple_of(step * WIDTH_ROWS + 8 * g, 8), 8)

            def load(n):
                lanes = slice(HIGH * n, HIGH * (n + 1))
                return (
                    x_ref[0, 0, 8 * g : 8 * g + 8, lanes],
                    x_ref[0, 1, 8 * g : 8 * g + 8, lanes],
                )

            def store(k, pair):
                cosine, sine = tw_ref[0, k : k + 1, :], tw_ref[1, k : k + 1, :]
                mid_ref[k, rows, 0:HIGH] = pair[0] * cosine - pair[1] * sine
                mid_ref[k, rows, HIGH:] = pair[0] * sine + pair[1] * cosine

            low_transform(load, store, part_ref.at[g], -1)

    @pl.when(step >= WIDTH_STEPS)
    def _():
        base = (step - WIDTH_STEPS) * WIDTH_LOWS
        for k in range(WIDTH_LOWS):
            flat = narrow_product(mid_ref[base + k], high_ref, both_ref).T
            out_ref[k, 0] = flat[: flat.shape[0] // 2]
            out_ref[k, 1] = flat[flat.shape[0] // 2 :]


def whole(*dims):
    return pl.BlockSpec(dims, lambda i: (0,) * len(dims))


def along_width(target, start, count):
    high, low = [
        np.concatenate(
            [table[:, start : start + count], table[:, HIGH + start : HIGH + start + count]], 1
        )
        for table in block_table(-1.0, 1.0 / 64)
    ]
    return pl.pallas_call(
        width_kernel,
        name="along_width",
        grid=(2 * WIDTH_STEPS,),
        in_specs=[
            pl.BlockSpec(
                (1, 2, WIDTH_ROWS, N), lambda i: (0, 0, jnp.minimum(i, WIDTH_STEPS - 1), 0)
            ),
            whole(2, LOW, HIGH),
            whole(2 * HIGH, HIGH),
            whole(2 * HIGH, 2 * HIGH),
        ],
        out_specs=pl.BlockSpec(
            (WIDTH_LOWS, 2, count, HIGH), lambda i: (jnp.maximum(i - WIDTH_STEPS, 0), 0, 0, 0)
        ),
        out_shape=jax.ShapeDtypeStruct((LOW, 2, count, HIGH), jnp.float32),
        scratch_shapes=[
            pltpu.VMEM((LOW, HIGH, 2 * HIGH), jnp.float32),
            pltpu.VMEM((WIDTH_ROWS // 8, LOW, 2, 8, HIGH), jnp.float32),
        ],
        cost_estimate=pl.CostEstimate(
            flops=6 * N * 512 * 2 * count, bytes_accessed=6 << 20, transcendentals=0
        ),
    )(
        target,
        jnp.asarray(twiddles(-1.0)),
        jnp.asarray(high),
        jnp.asarray(np.concatenate([high, low], 1)),
    )


HEIGHT_ROWS = 16


def height_kernel(x_ref, h_ref, ftw_ref, fh_ref, fl_ref, btw_ref, bh_ref, bl_ref,
                  out_ref, mid_ref, part_ref):
    groups = HEIGHT_ROWS // 8
    for g in range(groups):
        rows = slice(8 * g, 8 * g + 8)

        def load(n):
            return (x_ref[n, 0, rows, :], x_ref[n, 1, rows, :])

        def store(k, pair):
            cosine, sine = ftw_ref[0, k : k + 1, :], ftw_ref[1, k : k + 1, :]
            mid_ref[k, rows, 0:HIGH] = pair[0] * cosine - pair[1] * sine
            mid_ref[k, rows, HIGH:] = pair[0] * sine + pair[1] * cosine

        low_transform(load, store, part_ref.at[g], -1)

    count = 8
    for b in range(0, LOW, count):
        part = slice(b, b + count)
        flat = mid_ref[part].reshape(count * HEIGHT_ROWS, 2 * HIGH)
        spectrum = product(flat, (fh_ref, fl_ref))
        real, imaginary = spectrum[:, :HIGH], spectrum[:, HIGH:]
        cosine = h_ref[part, 0].reshape(count * HEIGHT_ROWS, HIGH)
        sine = h_ref[part, 1].reshape(count * HEIGHT_ROWS, HIGH)
        moved = jnp.concatenate(
            [real * cosine - imaginary * sine, real * sine + imaginary * cosine], axis=1
        )
        back = product(moved, (bh_ref, bl_ref))
        mid_ref[part] = back.reshape(count, HEIGHT_ROWS, 2 * HIGH)

    for g in range(groups):
        rows = slice(8 * g, 8 * g + 8)

        def load(k):
            real, imaginary = mid_ref[k, rows, 0:HIGH], mid_ref[k, rows, HIGH:]
            cosine, sine = btw_ref[0, k : k + 1, :], btw_ref[1, k : k + 1, :]
            return (real * cosine - imaginary * sine, real * sine + imaginary * cosine)

        def store(n, pair):
            out_ref[n, 0, rows, :] = pair[0]
            out_ref[n, 1, rows, :] = pair[1]

        low_transform(load, store, part_ref.at[g], 1)


def along_height(columns, transfer):
    count = columns.shape[2]
    spec = pl.BlockSpec((LOW, 2, HEIGHT_ROWS, HIGH), lambda i: (0, 0, i, 0))
    table = whole(2 * HIGH, 2 * HIGH)
    forward, backward = block_table(-1.0, 1.0 / 64), block_table(1.0, 1.0 / 64)
    return pl.pallas_call(
        height_kernel,
        name="along_height",
        compiler_params=pltpu.CompilerParams(vmem_limit_bytes=14 << 20),
        grid=(count // HEIGHT_ROWS,),
        in_specs=[spec, spec, whole(2, LOW, HIGH), table, table, whole(2, LOW, HIGH), table, table],
        out_specs=spec,
        out_shape=pltpu.HBM((LOW, 2, count, HIGH), jnp.float32),
        scratch_shapes=[
            pltpu.VMEM((LOW, HEIGHT_ROWS, 2 * HIGH), jnp.float32),
            pltpu.VMEM((HEIGHT_ROWS // 8, LOW, 2, 8, HIGH), jnp.float32),
        ],
        cost_estimate=pl.CostEstimate(
            flops=12 * LOW * count * 512 * 256,
            bytes_accessed=3 * 8 * LOW * count * HIGH,
            transcendentals=0,
        ),
    )(
        columns,
        transfer,
        jnp.asarray(twiddles(-1.0)),
        *[jnp.asarray(t) for t in forward],
        jnp.asarray(twiddles(1.0)),
        *[jnp.asarray(t) for t in backward],
    )


def flip_kernel(x_ref, out_ref):
    for n in range(4):
        tile = jnp.concatenate([x_ref[n, 0], x_ref[n, 1]], axis=0)
        out_ref[16 * n : 16 * n + 16] = tile.T.reshape(16, 8, HIGH)


def flip(share):
    return pl.pallas_call(
        flip_kernel,
        name="flip",
        compiler_params=pltpu.CompilerParams(vmem_limit_bytes=6 << 20),
        out_shape=jax.ShapeDtypeStruct((64, 8, HIGH), jnp.float32),
        cost_estimate=pl.CostEstimate(flops=1 << 18, bytes_accessed=1 << 19, transcendentals=0),
    )(pltpu.with_memory_space_constraint(share, pltpu.HBM))


def inverse_width_kernel(
    first_ref, second_ref, tw_ref, high_ref, low_ref, out_ref, mid_ref, part_ref
):
    rows = jnp.concatenate(
        [ref[0:LOW] + ref[LOW:] for ref in (first_ref, second_ref)], axis=-1
    ).reshape(LOW * 8, 2 * HIGH)
    mid_ref[...] = product(rows, (high_ref, low_ref)).reshape(LOW, 8, 2 * HIGH)

    def load(k):
        real, imaginary = mid_ref[k, :, 0:HIGH], mid_ref[k, :, HIGH:]
        cosine, sine = tw_ref[0, k : k + 1, :], tw_ref[1, k : k + 1, :]
        return (real * cosine - imaginary * sine, real * sine + imaginary * cosine)

    def store(n, pair):
        out_ref[0, :, HIGH * n : HIGH * (n + 1)] = pair[0]
        out_ref[1, :, HIGH * n : HIGH * (n + 1)] = pair[1]

    low_transform(load, store, part_ref, 1)


def inverse_width(pieces, scaling):
    high, low = [
        table.reshape(2, 2, HIGH // 2, 2 * HIGH).swapaxes(0, 1).reshape(table.shape)
        for table in block_table(1.0, scaling / 64)
    ]
    return pl.pallas_call(
        inverse_width_kernel,
        name="inverse_width",
        compiler_params=pltpu.CompilerParams(vmem_limit_bytes=8 << 20),
        out_shape=jax.ShapeDtypeStruct((2, 8, N), jnp.float32),
        scratch_shapes=[
            pltpu.VMEM((LOW, 8, 2 * HIGH), jnp.float32),
            pltpu.VMEM((LOW, 2, 8, HIGH), jnp.float32),
        ],
    )(*pieces, jnp.asarray(twiddles(1.0)), jnp.asarray(high), jnp.asarray(low))


def signed(natural):
    return jnp.where(natural < N // 2, natural, natural - N)


def transfer_factors(depth_index, band_mask, column, start, count):
    high = jnp.arange(HIGH, dtype=jnp.int32)
    low = jnp.arange(LOW, dtype=jnp.int32)
    height = signed(low[:, None] + LOW * high[None, :])
    width = signed(column + LOW * (start + jnp.arange(count, dtype=jnp.int32)))
    square = (height * height)[:, None, :] + (width * width)[None, :, None]
    square = square.astype(jnp.float32) * np.float32(1.0 / (N * N))
    descent = -square / (jnp.sqrt(4.0 - square) + 2.0)
    turns = (100.0 + 2.0 * depth_index[0].astype(jnp.float32)) * descent
    angles = np.float32(2.0 * math.pi) * (turns - jnp.round(turns))
    mask_height = band_mask[0, 0].reshape(HIGH, LOW).T.astype(jnp.float32)
    mask_width = lax.dynamic_slice_in_dim(
        band_mask[0, 1].reshape(HIGH, LOW).T, column, 1, 0
    )[0, start : start + count].astype(jnp.float32)
    weights = mask_height[:, None, :] * mask_width[None, :, None]
    return jnp.stack([jnp.cos(angles) * weights, jnp.sin(angles) * weights], axis=1)


def hologram(target, depth_index, band_mask):
    transfer = []
    for start, count in zip(STARTS, CHUNKS):
        column = lax.axis_index("rows")
        transfer.append(transfer_factors(depth_index, band_mask, column, start, count))
    pieces = []
    for i, (start, count) in enumerate(zip(STARTS, CHUNKS)):
        block = along_width(target, start, count)
        columns = lax.all_to_all(block, "rows", split_axis=0, concat_axis=0, tiled=True)
        part = along_height(columns, transfer[i])
        share = lax.psum_scatter(part, "depth_0", scatter_dimension=0, tiled=True)
        pieces.append(
            lax.all_to_all(
                flip(share), ("depth_1", "rows"), split_axis=0, concat_axis=0, tiled=True
            )
        )
    return inverse_width(pieces, 1.0 / math.sqrt(lax.axis_size(DEPTH)))


def solution(mesh):
    split = Mesh(mesh.devices.reshape(8, 2, mesh.shape["rows"]), ("depth_0", "depth_1", "rows"))
    in_specs = (P(DEPTH, None, "rows", None), P(DEPTH), P(DEPTH, None, None))
    out_specs = P(None, DEPTH_ROWS, None)
    return jax.shard_map(hologram, mesh=split, in_specs=in_specs, out_specs=out_specs, check_vma=False)
```

```python
import functools
import math

import jax
import jax.numpy as jnp
import numpy as np
from jax import lax
from jax.experimental import pallas as pl
from jax.experimental.pallas import tpu as pltpu
from jax.sharding import Mesh
from jax.sharding import PartitionSpec as P

LOW = 32
HIGH = 128
N = 4096
DEPTH = ("depth_0", "depth_1")
DEPTH_ROWS = ("depth_0", "depth_1", "rows")
CHUNKS = (64, 64)
STARTS = (0, 64)


def block_table(direction, scaling):
    index = np.arange(HIGH)
    angles = direction * 2.0 * np.pi / HIGH * (index[:, None] * index[None, :] % HIGH)
    cosine, sine = np.cos(angles) * scaling, np.sin(angles) * scaling
    table = np.concatenate(
        [np.concatenate([cosine, sine], 1), np.concatenate([-sine, cosine], 1)], 0
    ).astype(np.float32)
    high = table.astype(jnp.bfloat16)
    low = (table - high.astype(np.float32)).astype(jnp.bfloat16)
    return high, low


def twiddles(direction):
    product = np.arange(LOW)[:, None] * np.arange(HIGH)[None, :] % N
    angles = direction * 2.0 * np.pi / N * product
    return np.stack([np.cos(angles), np.sin(angles)]).astype(np.float32)


def add(a, b):
    return (a[0] + b[0], a[1] + b[1])


def sub(a, b):
    return (a[0] - b[0], a[1] - b[1])


def quarter(a, sign):
    return (-a[1], a[0]) if sign > 0 else (a[1], -a[0])


def turn(a, numerator, length, sign):
    numerator %= length
    if numerator == 0:
        return a
    if numerator * 4 == length:
        return quarter(a, sign)
    if numerator * 2 == length:
        return (-a[0], -a[1])
    if numerator * 8 == length:
        half = np.float32(math.sqrt(0.5))
        b = quarter(a, sign)
        return ((a[0] + b[0]) * half, (a[1] + b[1]) * half)
    if numerator * 8 == 3 * length:
        half = np.float32(math.sqrt(0.5))
        b = quarter(a, sign)
        return ((b[0] - a[0]) * half, (b[1] - a[1]) * half)
    angle = sign * 2.0 * math.pi * numerator / length
    cosine, sine = np.float32(math.cos(angle)), np.float32(math.sin(angle))
    return (a[0] * cosine - a[1] * sine, a[0] * sine + a[1] * cosine)


def four_points(values, sign):
    even, odd = add(values[0], values[2]), sub(values[0], values[2])
    even_2, odd_2 = add(values[1], values[3]), quarter(sub(values[1], values[3]), sign)
    return [add(even, even_2), add(odd, odd_2), sub(even, even_2), sub(odd, odd_2)]


def eight_points(values, sign):
    first = four_points(values[0::2], sign)
    second = four_points(values[1::2], sign)
    second = [turn(second[k], k, 8, sign) for k in range(4)]
    return [add(first[k], second[k]) for k in range(4)] + [
        sub(first[k], second[k]) for k in range(4)
    ]


def low_transform(load, store, part_ref, sign):
    for a in range(8):
        outs = four_points([load(a + 8 * b) for b in range(4)], sign)
        for q in range(4):
            pair = turn(outs[q], a * q, 32, sign)
            part_ref[q * 8 + a, 0] = pair[0]
            part_ref[q * 8 + a, 1] = pair[1]
    for q in range(4):
        values = [(part_ref[q * 8 + a, 0], part_ref[q * 8 + a, 1]) for a in range(8)]
        outs = eight_points(values, sign)
        for p in range(8):
            store(q + 4 * p, outs[p])


def product(rows, table):
    high_table, low_table = table[0][...], table[1][...]
    high = rows.astype(jnp.bfloat16)
    low = (rows - high.astype(jnp.float32)).astype(jnp.bfloat16)
    dot = functools.partial(jnp.dot, preferred_element_type=jnp.float32)
    return dot(high, high_table) + (dot(low, high_table) + dot(high, low_table))


WIDTH_ROWS = 32
WIDTH_STEPS = HIGH // WIDTH_ROWS
WIDTH_LOWS = LOW // WIDTH_STEPS


def narrow_product(rows, high_ref, both_ref):
    high = rows.astype(jnp.bfloat16)
    low = (rows - high.astype(jnp.float32)).astype(jnp.bfloat16)
    first = jnp.dot(high, both_ref[...], preferred_element_type=jnp.float32)
    second = jnp.dot(low, high_ref[...], preferred_element_type=jnp.float32)
    return first[:, :HIGH] + (first[:, HIGH:] + second)


def width_kernel(x_ref, tw_ref, high_ref, both_ref, out_ref, mid_ref, part_ref):
    step = pl.program_id(0)

    @pl.when(step < WIDTH_STEPS)
    def _():
        for g in range(WIDTH_ROWS // 8):
            rows = pl.ds(pl.multiple_of(step * WIDTH_ROWS + 8 * g, 8), 8)

            def load(n):
                lanes = slice(HIGH * n, HIGH * (n + 1))
                return (
                    x_ref[0, 0, 8 * g : 8 * g + 8, lanes],
                    x_ref[0, 1, 8 * g : 8 * g + 8, lanes],
                )

            def store(k, pair):
                cosine, sine = tw_ref[0, k : k + 1, :], tw_ref[1, k : k + 1, :]
                mid_ref[k, rows, 0:HIGH] = pair[0] * cosine - pair[1] * sine
                mid_ref[k, rows, HIGH:] = pair[0] * sine + pair[1] * cosine

            low_transform(load, store, part_ref.at[g], -1)

    @pl.when(step >= WIDTH_STEPS)
    def _():
        base = (step - WIDTH_STEPS) * WIDTH_LOWS
        for k in range(WIDTH_LOWS):
            flat = narrow_product(mid_ref[base + k], high_ref, both_ref).T
            out_ref[k, 0] = flat[: flat.shape[0] // 2]
            out_ref[k, 1] = flat[flat.shape[0] // 2 :]


def whole(*dims):
    return pl.BlockSpec(dims, lambda i: (0,) * len(dims))


def along_width(target, start, count):
    high, low = [
        np.concatenate(
            [table[:, start : start + count], table[:, HIGH + start : HIGH + start + count]], 1
        )
        for table in block_table(-1.0, 1.0 / 64)
    ]
    return pl.pallas_call(
        width_kernel,
        name="along_width",
        grid=(2 * WIDTH_STEPS,),
        in_specs=[
            pl.BlockSpec(
                (1, 2, WIDTH_ROWS, N), lambda i: (0, 0, jnp.minimum(i, WIDTH_STEPS - 1), 0)
            ),
            whole(2, LOW, HIGH),
            whole(2 * HIGH, HIGH),
            whole(2 * HIGH, 2 * HIGH),
        ],
        out_specs=pl.BlockSpec(
            (WIDTH_LOWS, 2, count, HIGH), lambda i: (jnp.maximum(i - WIDTH_STEPS, 0), 0, 0, 0)
        ),
        out_shape=jax.ShapeDtypeStruct((LOW, 2, count, HIGH), jnp.float32),
        scratch_shapes=[
            pltpu.VMEM((LOW, HIGH, 2 * HIGH), jnp.float32),
            pltpu.VMEM((WIDTH_ROWS // 8, LOW, 2, 8, HIGH), jnp.float32),
        ],
        cost_estimate=pl.CostEstimate(
            flops=6 * N * 512 * 2 * count, bytes_accessed=6 << 20, transcendentals=0
        ),
    )(
        target,
        jnp.asarray(twiddles(-1.0)),
        jnp.asarray(high),
        jnp.asarray(np.concatenate([high, low], 1)),
    )


HEIGHT_ROWS = 32


def height_kernel(x_ref, h_ref, ftw_ref, fh_ref, fl_ref, btw_ref, bh_ref, bl_ref,
                  out_ref, mid_ref, part_ref):
    groups = HEIGHT_ROWS // 8
    for g in range(groups):
        rows = slice(8 * g, 8 * g + 8)

        def load(n):
            return (x_ref[n, 0, rows, :], x_ref[n, 1, rows, :])

        def store(k, pair):
            cosine, sine = ftw_ref[0, k : k + 1, :], ftw_ref[1, k : k + 1, :]
            mid_ref[k, rows, 0:HIGH] = pair[0] * cosine - pair[1] * sine
            mid_ref[k, rows, HIGH:] = pair[0] * sine + pair[1] * cosine

        low_transform(load, store, part_ref.at[g], -1)

    count = 8
    for b in range(0, LOW, count):
        part = slice(b, b + count)
        flat = mid_ref[part].reshape(count * HEIGHT_ROWS, 2 * HIGH)
        spectrum = product(flat, (fh_ref, fl_ref))
        real, imaginary = spectrum[:, :HIGH], spectrum[:, HIGH:]
        cosine = h_ref[part, 0].reshape(count * HEIGHT_ROWS, HIGH)
        sine = h_ref[part, 1].reshape(count * HEIGHT_ROWS, HIGH)
        moved = jnp.concatenate(
            [real * cosine - imaginary * sine, real * sine + imaginary * cosine], axis=1
        )
        back = product(moved, (bh_ref, bl_ref))
        mid_ref[part] = back.reshape(count, HEIGHT_ROWS, 2 * HIGH)

    for g in range(groups):
        rows = slice(8 * g, 8 * g + 8)

        def load(k):
            real, imaginary = mid_ref[k, rows, 0:HIGH], mid_ref[k, rows, HIGH:]
            cosine, sine = btw_ref[0, k : k + 1, :], btw_ref[1, k : k + 1, :]
            return (real * cosine - imaginary * sine, real * sine + imaginary * cosine)

        def store(n, pair):
            out_ref[n, 0, rows, :] = pair[0]
            out_ref[n, 1, rows, :] = pair[1]

        low_transform(load, store, part_ref.at[g], 1)


def along_height(columns, transfer):
    count = columns.shape[2]
    spec = pl.BlockSpec((LOW, 2, HEIGHT_ROWS, HIGH), lambda i: (0, 0, i, 0))
    table = whole(2 * HIGH, 2 * HIGH)
    forward, backward = block_table(-1.0, 1.0 / 64), block_table(1.0, 1.0 / 64)
    return pl.pallas_call(
        height_kernel,
        name="along_height",
        compiler_params=pltpu.CompilerParams(vmem_limit_bytes=14 << 20),
        grid=(count // HEIGHT_ROWS,),
        in_specs=[spec, spec, whole(2, LOW, HIGH), table, table, whole(2, LOW, HIGH), table, table],
        out_specs=spec,
        out_shape=pltpu.HBM((LOW, 2, count, HIGH), jnp.float32),
        scratch_shapes=[
            pltpu.VMEM((LOW, HEIGHT_ROWS, 2 * HIGH), jnp.float32),
            pltpu.VMEM((HEIGHT_ROWS // 8, LOW, 2, 8, HIGH), jnp.float32),
        ],
        cost_estimate=pl.CostEstimate(
            flops=12 * LOW * count * 512 * 256,
            bytes_accessed=3 * 8 * LOW * count * HIGH,
            transcendentals=0,
        ),
    )(
        columns,
        transfer,
        jnp.asarray(twiddles(-1.0)),
        *[jnp.asarray(t) for t in forward],
        jnp.asarray(twiddles(1.0)),
        *[jnp.asarray(t) for t in backward],
    )


def flip_kernel(x_ref, out_ref):
    for n in range(4):
        tile = jnp.concatenate([x_ref[n, 0], x_ref[n, 1]], axis=0)
        out_ref[16 * n : 16 * n + 16] = tile.T.reshape(16, 8, HIGH)


def flip(share):
    return pl.pallas_call(
        flip_kernel,
        name="flip",
        compiler_params=pltpu.CompilerParams(vmem_limit_bytes=6 << 20),
        out_shape=jax.ShapeDtypeStruct((64, 8, HIGH), jnp.float32),
        cost_estimate=pl.CostEstimate(flops=1 << 18, bytes_accessed=1 << 19, transcendentals=0),
    )(pltpu.with_memory_space_constraint(share, pltpu.HBM))


def inverse_width_kernel(
    first_ref, second_ref, tw_ref, high_ref, low_ref, out_ref, mid_ref, part_ref
):
    rows = jnp.concatenate(
        [ref[0:LOW] + ref[LOW:] for ref in (first_ref, second_ref)], axis=-1
    ).reshape(LOW * 8, 2 * HIGH)
    mid_ref[...] = product(rows, (high_ref, low_ref)).reshape(LOW, 8, 2 * HIGH)

    def load(k):
        real, imaginary = mid_ref[k, :, 0:HIGH], mid_ref[k, :, HIGH:]
        cosine, sine = tw_ref[0, k : k + 1, :], tw_ref[1, k : k + 1, :]
        return (real * cosine - imaginary * sine, real * sine + imaginary * cosine)

    def store(n, pair):
        out_ref[0, :, HIGH * n : HIGH * (n + 1)] = pair[0]
        out_ref[1, :, HIGH * n : HIGH * (n + 1)] = pair[1]

    low_transform(load, store, part_ref, 1)


def inverse_width(pieces, scaling):
    high, low = [
        table.reshape(2, 2, HIGH // 2, 2 * HIGH).swapaxes(0, 1).reshape(table.shape)
        for table in block_table(1.0, scaling / 64)
    ]
    return pl.pallas_call(
        inverse_width_kernel,
        name="inverse_width",
        compiler_params=pltpu.CompilerParams(vmem_limit_bytes=8 << 20),
        out_shape=jax.ShapeDtypeStruct((2, 8, N), jnp.float32),
        scratch_shapes=[
            pltpu.VMEM((LOW, 8, 2 * HIGH), jnp.float32),
            pltpu.VMEM((LOW, 2, 8, HIGH), jnp.float32),
        ],
    )(*pieces, jnp.asarray(twiddles(1.0)), jnp.asarray(high), jnp.asarray(low))


def signed(natural):
    return jnp.where(natural < N // 2, natural, natural - N)


def transfer_factors(depth_index, band_mask, column, start, count):
    high = jnp.arange(HIGH, dtype=jnp.int32)
    low = jnp.arange(LOW, dtype=jnp.int32)
    height = signed(low[:, None] + LOW * high[None, :])
    width = signed(column + LOW * (start + jnp.arange(count, dtype=jnp.int32)))
    square = (height * height)[:, None, :] + (width * width)[None, :, None]
    square = square.astype(jnp.float32) * np.float32(1.0 / (N * N))
    descent = -square / (jnp.sqrt(4.0 - square) + 2.0)
    turns = (100.0 + 2.0 * depth_index[0].astype(jnp.float32)) * descent
    angles = np.float32(2.0 * math.pi) * (turns - jnp.round(turns))
    mask_height = band_mask[0, 0].reshape(HIGH, LOW).T.astype(jnp.float32)
    mask_width = lax.dynamic_slice_in_dim(
        band_mask[0, 1].reshape(HIGH, LOW).T, column, 1, 0
    )[0, start : start + count].astype(jnp.float32)
    weights = mask_height[:, None, :] * mask_width[None, :, None]
    return jnp.stack([jnp.cos(angles) * weights, jnp.sin(angles) * weights], axis=1)


def hologram(target, depth_index, band_mask):
    transfer = []
    for start, count in zip(STARTS, CHUNKS):
        column = lax.axis_index("rows")
        factors = transfer_factors(depth_index, band_mask, column, start, count)
        if start == 0:
            factors = pltpu.with_memory_space_constraint(factors, pltpu.HBM)
        transfer.append(factors)
    pieces = []
    for i, (start, count) in enumerate(zip(STARTS, CHUNKS)):
        block = along_width(target, start, count)
        columns = lax.all_to_all(block, "rows", split_axis=0, concat_axis=0, tiled=True)
        part = along_height(columns, transfer[i])
        share = lax.psum_scatter(part, "depth_0", scatter_dimension=0, tiled=True)
        pieces.append(
            lax.all_to_all(
                flip(share), ("depth_1", "rows"), split_axis=0, concat_axis=0, tiled=True
            )
        )
    return inverse_width(pieces, 1.0 / math.sqrt(lax.axis_size(DEPTH)))


def solution(mesh):
    split = Mesh(mesh.devices.reshape(8, 2, mesh.shape["rows"]), ("depth_0", "depth_1", "rows"))
    in_specs = (P(DEPTH, None, "rows", None), P(DEPTH), P(DEPTH, None, None))
    out_specs = P(None, DEPTH_ROWS, None)
    return jax.shard_map(hologram, mesh=split, in_specs=in_specs, out_specs=out_specs, check_vma=False)
```
